256 devices in a mesh: layer: 8 (over z), row: 16 (over y, x), col: 2 (over core).
Axes of the slice: x: 4, y: 4, z: 8, core: 2. Of those that a mesh axis runs over, the one named last changes fastest.
Arguments:
- leaf_rhs: float32 [8, 3, 4096, 256], P('layer', None, 'row'), may hold values from -6 to 6
- anc_rhs: float32 [2, 4096, 256], P(None, 'row'), may hold values from -6 to 6
- leaf_tiles: bfloat16 [8, 3, 4096, 4096], P('layer', None, 'row', 'col'), may hold values from -0.09375 to 0.09375
- cross_tiles: bfloat16 [8, 2, 3, 4096, 4096], P('layer', None, None, 'row', 'col'), may hold values from -0.03125 to 0.03125
- top_tiles: bfloat16 [1, 4096, 4096], P(None, 'row', 'col'), may hold values from -0.09375 to 0.09375
- leaf_pattern: int32 [8, 3, 32, 32], P('layer', None, 'row', 'col'), may hold values 0 or 1
- cross_pattern: int32 [8, 2, 3, 32, 32], P('layer', None, None, 'row', 'col'), may hold values 0 or 1
- top_pattern: int32 [1, 32, 32], P(None, 'row', 'col'), may hold values 0 or 1
- leaf_inverse: bfloat16 [8, 3, 32, 128, 128], P('layer'), may hold values from -0.5 to 0.5
- anc_inverse: bfloat16 [2, 32, 128, 128], replicated, may hold values from -0.5 to 0.5
Outputs:
- leaf_solution: bfloat16 [8, 3, 4096, 256], P('layer', None, 'row')
- anc_solution: bfloat16 [2, 4096, 256], P(None, 'row')
The draws below stay inside these ranges and needn't reach their ends.
All inputs are finite; a program needn't handle non-finite values. No bound on the sum of `leaf_pattern` or of `cross_pattern` or of `top_pattern` on one device may be relied on, other than what follows from the above.
Results may differ from the reference program's by a relative error of at most 0.023.
Values may be sent and summed in bfloat16 or wider, within the bound.
No kernel may reach another device: no remote copies, remote signals or barrier semaphores. Data moves between devices by JAX's collectives and lax.ppermute only.
A program may use at most 128 MiB of HBM per device.

```python
import jax
import jax.numpy as jnp
from jax import lax

TILE = 128
NRHS = 256
LEAF_LEV = 3
ANC_LEV = 2
NSUP = 32
NODES = 4096
LEAF_PAIRS = 3
ANC_PAIRS = 1
N_LAYER = 8


def set_ends(drawn, stream_key, low, top_value):
    longest = drawn.shape.index(max(drawn.shape))
    spots = []
    for shift in (0, 1):
        where = [jax.random.randint(jax.random.fold_in(stream_key, axis), (), 0, length) for axis, length in enumerate(drawn.shape)]
        where[longest] = (where[longest] + shift) % drawn.shape[longest]
        spots.append(tuple(where))
    return drawn.at[spots[0]].set(low).at[spots[1]].set(top_value)


def shard_levels(own_key, dims, cuts, least, top_value):
    def one(dim, parts):
        steps = jax.random.uniform(jax.random.fold_in(jax.random.fold_in(own_key, 6), dim), (parts,), jnp.float32, least / len(cuts), top_value / len(cuts))
        return jnp.repeat(jnp.exp(steps), dims[dim] // parts).reshape((-1,) + (1,) * (len(dims) - dim - 1))

    loudness = one(*cuts[0])
    for cut in cuts[1:]:
        loudness = loudness * one(*cut)
    return loudness


def normal_values(rng, dims, deviation, bound, cuts=(), held_as=jnp.bfloat16):
    values = deviation * jax.random.normal(rng, dims, jnp.float32)
    if cuts:
        values = values * shard_levels(rng, dims, cuts, -0.22, 0.18)
    return jnp.clip(values, -bound, bound).astype(held_as)


def setup_inputs(seed: int = 0) -> dict:
    key_of = jax.random.split(jax.random.key(seed), 11)
    return {
        "leaf_rhs": normal_values(key_of[0], (N_LAYER, LEAF_LEV, NODES, NRHS), 1.0, 6.0, ((0, 8), (2, 16)), jnp.float32),
        "anc_rhs": normal_values(key_of[1], (ANC_LEV, NODES, NRHS), 1.0, 6.0, ((1, 16),), jnp.float32),
        "leaf_tiles": normal_values(key_of[2], (N_LAYER, LEAF_PAIRS, NODES, NODES), NODES ** -0.5, 0.09375, ((0, 8), (2, 16), (3, 2))),
        "cross_tiles": normal_values(key_of[3], (N_LAYER, ANC_LEV, LEAF_LEV, NODES, NODES), (NODES * N_LAYER) ** -0.5, 0.03125, ((0, 8), (3, 16), (4, 2))),
        "top_tiles": normal_values(key_of[4], (ANC_PAIRS, NODES, NODES), NODES ** -0.5, 0.09375, ((1, 16), (2, 2))),
        "leaf_pattern": set_ends((jax.random.randint(key_of[5], (N_LAYER, LEAF_PAIRS, NSUP, NSUP), 0, 2) < 1).astype(jnp.int32), jax.random.fold_in(key_of[5], 1), 0, 1),
        "cross_pattern": set_ends((jax.random.randint(key_of[6], (N_LAYER, ANC_LEV, LEAF_LEV, NSUP, NSUP), 0, 2) < 1).astype(jnp.int32), jax.random.fold_in(key_of[6], 1), 0, 1),
        "top_pattern": set_ends((jax.random.randint(key_of[7], (ANC_PAIRS, NSUP, NSUP), 0, 2) < 1).astype(jnp.int32), jax.random.fold_in(key_of[7], 1), 0, 1),
        "leaf_inverse": normal_values(key_of[8], (N_LAYER, LEAF_LEV, NSUP, TILE, TILE), TILE ** -0.5, 0.5, ((0, 8),)),
        "anc_inverse": normal_values(key_of[9], (ANC_LEV, NSUP, TILE, TILE), TILE ** -0.5, 0.5),
    }


def pair_index(target, source):
    return target * (target - 1) // 2 + source


def product(pattern, tiles, vector, flipped):
    grown = jnp.repeat(jnp.repeat(pattern, TILE, axis=0), TILE, axis=1)
    dense = (tiles * grown.astype(tiles.dtype)).astype(jnp.float32)
    values = vector.astype(jnp.float32)
    if flipped:
        return jnp.dot(dense.T, values, precision=lax.Precision.HIGHEST)
    return jnp.dot(dense, values, precision=lax.Precision.HIGHEST)


def solve_blocks(inverse, residual, flipped):
    rounded = lax.optimization_barrier(residual.astype(jnp.bfloat16))
    pieces = rounded.astype(jnp.float32).reshape(NSUP, TILE, NRHS)
    text_form = "sji,sjk->sik" if flipped else "sij,sjk->sik"
    solved = jnp.einsum(text_form, inverse.astype(jnp.float32), pieces, precision=lax.Precision.HIGHEST)
    return solved.reshape(NODES, NRHS).astype(jnp.bfloat16)


def reference(leaf_rhs, anc_rhs, leaf_tiles, cross_tiles, top_tiles, leaf_pattern, cross_pattern, top_pattern, leaf_inverse, anc_inverse):
    layer_total = leaf_rhs.shape[0]
    forward_leaf = []
    for layer_number in range(layer_total):
        solved_levels = []
        for target in range(LEAF_LEV):
            summed = jnp.zeros((NODES, NRHS), jnp.float32)
            for source in range(target):
                pair_slot = pair_index(target, source)
                summed = summed + product(leaf_pattern[layer_number, pair_slot], leaf_tiles[layer_number, pair_slot], solved_levels[source], False)
            solved_levels.append(solve_blocks(leaf_inverse[layer_number, target], leaf_rhs[layer_number, target] - summed, False))
        forward_leaf.append(solved_levels)
    forward_anc = []
    for target in range(ANC_LEV):
        summed = jnp.zeros((NODES, NRHS), jnp.float32)
        for layer_number in range(layer_total):
            for source in range(LEAF_LEV):
                summed = summed + product(cross_pattern[layer_number, target, source], cross_tiles[layer_number, target, source], forward_leaf[layer_number][source], False)
        for source in range(target):
            pair_slot = pair_index(target, source)
            summed = summed + product(top_pattern[pair_slot], top_tiles[pair_slot], forward_anc[source], False)
        forward_anc.append(solve_blocks(anc_inverse[target], anc_rhs[target] - summed, False))
    anc_out = [None] * ANC_LEV
    for target in range(ANC_LEV - 1, -1, -1):
        summed = jnp.zeros((NODES, NRHS), jnp.float32)
        for source in range(target + 1, ANC_LEV):
            pair_slot = pair_index(source, target)
            summed = summed + product(top_pattern[pair_slot], top_tiles[pair_slot], anc_out[source], True)
        anc_out[target] = solve_blocks(anc_inverse[target], forward_anc[target].astype(jnp.float32) - summed, True)
    leaf_out = []
    for layer_number in range(layer_total):
        level_out = [None] * LEAF_LEV
        for target in range(LEAF_LEV - 1, -1, -1):
            summed = jnp.zeros((NODES, NRHS), jnp.float32)
            for upper in range(ANC_LEV):
                summed = summed + product(cross_pattern[layer_number, upper, target], cross_tiles[layer_number, upper, target], anc_out[upper], True)
            for source in range(target + 1, LEAF_LEV):
                pair_slot = pair_index(source, target)
                summed = summed + product(leaf_pattern[layer_number, pair_slot], leaf_tiles[layer_number, pair_slot], level_out[source], True)
            level_out[target] = solve_blocks(leaf_inverse[layer_number, target], forward_leaf[layer_number][target].astype(jnp.float32) - summed, True)
        leaf_out.append(jnp.stack(level_out))
    return jnp.stack(leaf_out), jnp.stack(anc_out)
```

```python
import functools

import jax
import jax.numpy as jnp
from jax import lax
from jax.experimental import pallas as pl
from jax.experimental.pallas import tpu as pltpu
from jax.sharding import PartitionSpec as P

F32 = jnp.float32
BF16 = jnp.bfloat16
TILE = 128
SWAP = [(0, 1), (1, 0)]

VMEM = pl.BlockSpec(memory_space=pltpu.VMEM)
SMEM = pl.BlockSpec(memory_space=pltpu.SMEM)


def nt(a, b):
    return lax.dot_general(a, b, (((1,), (1,)), ((), ())), preferred_element_type=F32)


def nn(a, b):
    return jnp.dot(a, b, preferred_element_type=F32)


def masked(tiles, pattern, slab, block):
    lines = []
    for upper in range(2):
        row = []
        for side in range(2):
            at = 2 * block + side
            tile = tiles[slab, TILE * upper : TILE * (upper + 1), TILE * at : TILE * (at + 1)]
            kept = pattern[(slab * 2 + upper) * 16 + at] != 0
            row.append(lax.select(kept, tile, jnp.zeros_like(tile)))
        lines.append(jnp.concatenate(row, axis=1))
    return jnp.concatenate(lines, axis=0)


def halves(where, own, other):
    return ((own, 0, where[0] * 8), (other, 1, (1 - where[0]) * 8))


def solved(residual, inverse):
    cut = residual.astype(BF16)
    return jnp.concatenate(
        [nt(cut[:, TILE * s : TILE * (s + 1)], inverse[s]) for s in range(2)], axis=1
    ).astype(BF16)


def solved_back(residual, inverse):
    cut = residual.astype(BF16)
    return jnp.concatenate(
        [nn(cut[:, TILE * s : TILE * (s + 1)], inverse[s]) for s in range(2)], axis=1
    ).astype(BF16)


def forward_sum(where, tiles, patterns, slab, values):
    total = None
    for half in range(2):
        first = (where[0] if half == 0 else 1 - where[0]) * 8
        for block in range(8):
            term = nt(values[first + block], masked(tiles[half], patterns[half], slab, block))
            total = term if total is None else total + term
    return total


def to_copies(out, value):
    for peer in range(out.shape[0]):
        out[peer] = value


def total_of(pieces):
    total = pieces[0].astype(F32)
    for peer in range(1, pieces.shape[0]):
        total = total + pieces[peer].astype(F32)
    return total


def call(body, out_shape, operands, flops, name):
    specs = [SMEM if x.dtype == jnp.int32 else VMEM for x in operands]
    single = not isinstance(out_shape, (list, tuple))
    shapes = [out_shape] if single else list(out_shape)
    moved = sum(x.size * x.dtype.itemsize for x in operands)
    out = pl.pallas_call(
        body,
        out_shape=shapes,
        in_specs=specs,
        out_specs=[VMEM] * len(shapes),
        compiler_params=pltpu.CompilerParams(vmem_limit_bytes=24 * 1024 * 1024),
        cost_estimate=pl.CostEstimate(flops=flops, bytes_accessed=moved, transcendentals=0),
        name=name,
    )(*operands)
    return out[0] if single else out


def shape(*dims, dtype=BF16):
    return jax.ShapeDtypeStruct(dims, dtype)


SLAB_FLOPS = 2 * 256 * 4096 * 128


def first_kernel(rhs, inverse, out):
    to_copies(out, solved(rhs[...].T, inverse))


def next_kernel(slabs, slab_of_last, *refs):
    where, pat_own, pat_oth, own, oth, values, rhs, inverse, *rest = refs
    out = rest[-1]
    total = forward_sum(where, (own, oth), (pat_own, pat_oth), slab_of_last, values)
    if len(rest) > 1:
        total = total + rest[0][...]
    to_copies(out, solved(rhs[...].T - total, inverse))


def part_kernel(slabs, where, pat_own, pat_oth, own, oth, values, out):
    for at, slab in enumerate(slabs):
        out[at] = forward_sum(where, (own, oth), (pat_own, pat_oth), slab, values)


def more_kernel(slabs, where, pat_own, pat_oth, own, oth, values, before, out):
    for at, slab in enumerate(slabs):
        out[at] = before[at] + forward_sum(where, (own, oth), (pat_own, pat_oth), slab, values)


def cross_kernel(slabs, where, pat_own, pat_oth, own, oth, values, before, out):
    layers = out.shape[0]
    for at, slab in enumerate(slabs):
        total = before[at] + forward_sum(where, (own, oth), (pat_own, pat_oth), slab, values)
        total = total.astype(BF16).reshape(layers, -1, total.shape[1])
        out[:, at] = total


def anc_first_kernel(pieces, rhs, inverse, out, rest):
    value = solved(rhs[0] - total_of(pieces.at[:, 0]), inverse)
    to_copies(out, value)
    rest[...] = rhs[1] - total_of(pieces.at[:, 1])


def anc_second_kernel(where, pat_own, pat_oth, own, oth, values, rest, inverse, out, top):
    total = forward_sum(where, (own, oth), (pat_own, pat_oth), 0, values)
    value = solved(rest[...] - total, inverse)
    back = solved_back(value.astype(F32), inverse)
    top[...] = back
    for half, tiles in enumerate((own, oth)):
        pattern = (pat_own, pat_oth)[half]
        first = (where[0] if half == 0 else 1 - where[0]) * 8
        for block in range(8):
            out[first + block] = nn(back, masked(tiles, pattern, 0, block)).astype(BF16)


def anc_third_kernel(row, pieces, lower, top, inverse, out):
    residual = lower[row[0]].astype(F32) - total_of(pieces)
    value = solved_back(residual, inverse)
    for peer in range(out.shape[0]):
        out[peer, 0] = value
        out[peer, 1] = top[...]


def back_parts(where, groups, out):
    for half in range(2):
        first = (where[0] if half == 0 else 1 - where[0]) * 8
        for block in range(8):
            total = None
            for tiles, patterns, slab, values in groups:
                term = nn(values, masked(tiles[half], patterns[half], slab, block))
                total = term if total is None else total + term
            out[first + block] = total.astype(BF16)


def of_layers(pieces, at):
    value = pieces[:, at]
    return value.reshape(-1, value.shape[-1])


def back_first_kernel(slabs, where, pat_own, pat_oth, own, oth, anc, out):
    groups = [
        ((own, oth), (pat_own, pat_oth), slab, of_layers(anc, at)) for at, slab in enumerate(slabs)
    ]
    back_parts(where, groups, out)


def back_next_kernel(
    cross_slabs, leaf_slabs, row, where, cpat_own, cpat_oth, lpat_own, lpat_oth, cown, coth, lown, loth,
    anc, pieces, value, inverse, *rest
):
    *earlier, out, solution, flipped = rest
    now = solved_back(value[row[0]].astype(F32) - total_of(pieces), inverse)
    solution[...] = now
    flipped[...] = now.astype(F32).T.astype(BF16)
    groups = [
        ((cown, coth), (cpat_own, cpat_oth), slab, of_layers(anc, at))
        for at, slab in enumerate(cross_slabs)
    ]
    known = [now, *(e[...] for e in earlier)]
    groups += [
        ((lown, loth), (lpat_own, lpat_oth), slab, values)
        for slab, values in zip(leaf_slabs, known)
    ]
    back_parts(where, groups, out)


def back_last_kernel(row, pieces, value, inverse, flipped):
    now = solved_back(value[row[0]].astype(F32) - total_of(pieces), inverse)
    flipped[...] = now.astype(F32).T.astype(BF16)


def flip_kernel(anc, out):
    for at in range(2):
        out[at] = of_layers(anc, at).astype(F32).T.astype(BF16)


def spread(x, axis):
    return lax.all_to_all(x, axis, split_axis=0, concat_axis=0, tiled=True)


def local(
    leaf_rhs, anc_rhs, leaf_tiles, cross_tiles, top_tiles, leaf_pattern, cross_pattern, top_pattern,
    leaf_inverse, anc_inverse,
):
    row = lax.axis_index("row")
    col = lax.axis_index("col")
    layer = lax.axis_index("layer")
    layers = lax.axis_size("layer")
    rows = lax.axis_size("row")
    leaf_own = leaf_tiles[0]
    cross_own = cross_tiles[0].reshape(6, 256, 2048)
    top_own = top_tiles
    patterns = jnp.concatenate(
        [leaf_pattern.reshape(-1), cross_pattern.reshape(-1), top_pattern.reshape(-1)]
    )
    pat_other = lax.ppermute(patterns, "col", SWAP)
    leaf_oth = lax.ppermute(leaf_own, "col", SWAP)
    cross_oth = lax.ppermute(cross_own, "col", SWAP)
    top_oth = lax.ppermute(top_own, "col", SWAP)
    lp = (patterns[:96], pat_other[:96])
    cp = (patterns[96:288], pat_other[96:288])
    tp = (patterns[288:], pat_other[288:])
    leaf_args = (*lp, leaf_own, leaf_oth)
    cross_args = (*cp, cross_own, cross_oth)
    top_args = (*tp, top_own, top_oth)
    where = col.astype(jnp.int32).reshape(1)
    here = row.astype(jnp.int32).reshape(1)

    rhs = lax.dynamic_slice_in_dim(leaf_rhs[0], col * 128, 128, 2)
    width = 128 // layers
    anc_part = lax.dynamic_slice_in_dim(anc_rhs, col * 128 + layer * width, width, 2).swapaxes(1, 2)
    inverse = lax.dynamic_slice_in_dim(leaf_inverse[0], 2 * row, 2, 1)
    inverse_anc = lax.dynamic_slice_in_dim(anc_inverse, 2 * row, 2, 1)

    wide = shape(rows, 128, 256)
    y0 = spread(call(first_kernel, wide, (rhs[0], inverse[0]), 1, "y0"), "row")
    y1 = spread(
        call(
            functools.partial(next_kernel, None, 0), wide, (where, *leaf_args, y0, rhs[1], inverse[1]), SLAB_FLOPS, "y1"
        ),
        "row",
    )
    part2 = call(
        functools.partial(part_kernel, (1,)), shape(1, 128, 256, dtype=F32), (where, *leaf_args, y0), SLAB_FLOPS, "p2"
    )[0]
    cross0 = call(
        functools.partial(part_kernel, (0, 3)), shape(2, 128, 256, dtype=F32), (where, *cross_args, y0), 2 * SLAB_FLOPS, "c0"
    )
    y2 = spread(
        call(
            functools.partial(next_kernel, None, 2), wide, (where, *leaf_args, y1, rhs[2], inverse[2], part2), SLAB_FLOPS, "y2"
        ),
        "row",
    )
    cross1 = call(
        functools.partial(more_kernel, (1, 4)), shape(2, 128, 256, dtype=F32), (where, *cross_args, y1, cross0), 2 * SLAB_FLOPS, "c1"
    )
    lower = spread(
        call(
            functools.partial(cross_kernel, (2, 5)), shape(layers, 2, width, 256), (where, *cross_args, y2, cross1), 2 * SLAB_FLOPS, "c2"
        ),
        "layer",
    )
    z0, rest = call(
        anc_first_kernel, [shape(rows, width, 256), shape(width, 256, dtype=F32)], (lower, anc_part, inverse_anc[0]), 1, "z0"
    )
    z0 = spread(z0, "row")
    pieces, top = call(
        anc_second_kernel, [shape(rows, width, 256), shape(width, 256)], (where, *top_args, z0, rest, inverse_anc[1]), SLAB_FLOPS // 4, "z1"
    )
    pieces = spread(pieces, "row")
    anc = call(
        anc_third_kernel, shape(layers, 2, width, 256), (here, pieces, z0, top, inverse_anc[0]), 1, "a0"
    )
    anc = spread(anc, "layer")
    pieces = spread(
        call(functools.partial(back_first_kernel, (2, 5)), wide, (where, *cross_args, anc), 2 * SLAB_FLOPS, "b2"), "row"
    )
    flat = (shape(128, 256), shape(256, 128))
    both = (*cp, *lp, cross_own, cross_oth, leaf_own, leaf_oth)
    pieces, x2, f2 = call(
        functools.partial(back_next_kernel, (1, 4), (2,)), [wide, *flat],
        (here, where, *both, anc, pieces, y2, inverse[2]), 3 * SLAB_FLOPS, "b1",
    )
    pieces = spread(pieces, "row")
    pieces, x1, f1 = call(
        functools.partial(back_next_kernel, (0, 3), (0, 1)), [wide, *flat],
        (here, where, *both, anc, pieces, y1, inverse[1], x2), 4 * SLAB_FLOPS, "b0",
    )
    pieces = spread(pieces, "row")
    f0 = call(back_last_kernel, shape(256, 128), (here, pieces, y0, inverse[0]), 1, "x0")
    fa = call(flip_kernel, shape(2, 256, 128), (anc,), 1, "fa")

    def joined(mine):
        theirs = lax.ppermute(mine, "col", SWAP)
        return jnp.where(
            col == 0,
            jnp.concatenate([mine, theirs], axis=-1),
            jnp.concatenate([theirs, mine], axis=-1),
        )

    return (jnp.stack([joined(f0), joined(f1), joined(f2)])[None], joined(fa))


def solution(mesh):
    in_specs = (
        P("layer", None, "row", None),
        P(None, "row", None),
        P("layer", None, "row", "col"),
        P("layer", None, None, "row", "col"),
        P(None, "row", "col"),
        P("layer", None, "row", "col"),
        P("layer", None, None, "row", "col"),
        P(None, "row", "col"),
        P("layer", None, None, None, None),
        P(),
    )
    out_specs = (P("layer", None, "row", None), P(None, "row", None))
    return jax.shard_map(local, mesh=mesh, in_specs=in_specs, out_specs=out_specs, check_vma=False)
```

```python
import functools

import jax
import jax.numpy as jnp
from jax import lax
from jax.experimental import pallas as pl
from jax.experimental.pallas import tpu as pltpu
from jax.sharding import PartitionSpec as P

F32 = jnp.float32
BF16 = jnp.bfloat16
TILE = 128
SWAP = [(0, 1), (1, 0)]
SLAB_FLOPS = 2 * 256 * 4096 * 128
LEAF, CROSS, TOP = 0, 96, 288

VMEM = pl.BlockSpec(memory_space=pltpu.VMEM)
SMEM = pl.BlockSpec(memory_space=pltpu.SMEM)
HBM = pl.BlockSpec(memory_space=pltpu.HBM)


def nt(a, b):
    return lax.dot_general(a, b, (((1,), (1,)), ((), ())), preferred_element_type=F32)


def nn(a, b):
    return jnp.dot(a, b, preferred_element_type=F32)


class Slab:
    def __init__(self, refs, buffer, sems, index, place):
        self.patterns, self.first = refs[2:4], refs[4] + index * 32
        self.sources = [buffer.at[place, half] for half in range(2)]
        self.copies = [
            pltpu.make_async_copy(refs[half].at[index], buffer.at[place, half], sems.at[place, half])
            for half in range(2)
            if refs[4] != LEAF or half == 0
        ]
        if refs[4] == LEAF:
            self.sources[1] = refs[1].at[index]
        for copy in self.copies:
            copy.start()

    def wait(self):
        for copy in self.copies:
            copy.wait()

    def tile(self, half, upper, at):
        tile = self.sources[half][TILE * upper : TILE * (upper + 1), TILE * at : TILE * (at + 1)]
        kept = self.patterns[half][self.first + 16 * upper + at] != 0
        return lax.select(kept, tile, jnp.zeros_like(tile))

    def block(self, half, block):
        return jnp.concatenate(
            [
                jnp.concatenate([self.tile(half, u, 2 * block + s) for s in range(2)], axis=1)
                for u in range(2)
            ],
            axis=0,
        )

    def line(self, half):
        return jnp.concatenate([self.block(half, b) for b in range(8)], axis=1)


def first_block(where, half):
    return (where[1] if half == 0 else 1 - where[1]) * 8


def product(where, slab, values):
    total = None
    for half in range(2):
        first = pl.multiple_of(first_block(where, half) * 256, 2048)
        term = nn(slab.line(half), values[pl.ds(first, 2048), :])
        total = term if total is None else total + term
    return total


def solved(inverse, residual):
    cut = residual.astype(BF16)
    return jnp.concatenate(
        [nn(inverse[s], cut[TILE * s : TILE * (s + 1)]) for s in range(2)], axis=0
    ).astype(BF16)


def solved_flat(inverse, residual):
    cut = residual.astype(BF16)
    return jnp.concatenate(
        [nt(cut[:, TILE * s : TILE * (s + 1)], inverse[s]) for s in range(2)], axis=1
    ).astype(BF16)


def solved_back(inverse, residual):
    cut = residual.astype(BF16)
    return jnp.concatenate(
        [nn(cut[:, TILE * s : TILE * (s + 1)], inverse[s]) for s in range(2)], axis=1
    ).astype(BF16)


def to_copies(out, value):
    for peer in range(out.shape[0]):
        out[peer] = value


def total_of(pieces):
    total = pieces[0].astype(F32)
    for peer in range(1, pieces.shape[0]):
        total = total + pieces[peer].astype(F32)
    return total


def flipped(value):
    return value.astype(F32).T


def fetch(source, target, sem):
    copy = pltpu.make_async_copy(source, target, sem)
    copy.start()
    return copy


def own_inverse(where, inverse, level, target, sem):
    return fetch(inverse.at[level, pl.ds(2 * where[0], 2)], target, sem)


def own_columns(where, rhs, level, target, sem):
    return fetch(rhs.at[level, :, pl.ds(pl.multiple_of(where[1] * 128, 128), 128)], target, sem)


def forward_kernel(level, slabs, where, own, oth, pat_own, pat_oth, rhs, inverse, *rest):
    *values, out, buffer, sems, rhs_here, inv_here, sem = rest
    small = [
        own_columns(where, rhs, level, rhs_here, sem.at[0]),
        own_inverse(where, inverse, level, inv_here, sem.at[1]),
    ]
    refs = (own, oth, pat_own, pat_oth, LEAF)
    moving = [Slab(refs, buffer, sems, index, place) for place, index in enumerate(slabs)]
    for copy in small:
        copy.wait()
    residual = rhs_here[...]
    for slab, value in zip(moving, values):
        slab.wait()
        residual = residual - product(where, slab, value)
    to_copies(out, solved(inv_here, residual))


def first_kernel(where, rhs, inverse, out, rhs_here, inv_here, sem):
    small = [
        own_columns(where, rhs, 0, rhs_here, sem.at[0]),
        own_inverse(where, inverse, 0, inv_here, sem.at[1]),
    ]
    for copy in small:
        copy.wait()
    to_copies(out, solved(inv_here, rhs_here[...]))


def cross_kernel(where, own, oth, pat_own, pat_oth, *rest):
    *values, out, buffer, sems = rest
    layers, levels, width, _ = out.shape
    refs = (own, oth, pat_own, pat_oth, CROSS)
    order = [(a, s) for s in range(len(values)) for a in range(levels)]
    moving = [
        Slab(refs, buffer, sems, a * len(values) + s, place) for place, (a, s) in enumerate(order)
    ]
    totals = [None] * levels
    for slab, (a, s) in zip(moving, order):
        slab.wait()
        term = product(where, slab, values[s])
        totals[a] = term if totals[a] is None else totals[a] + term
    for a in range(levels):
        out[:, a] = totals[a].T.astype(BF16).reshape(layers, width, -1)


def anc_first_kernel(where, pieces, rhs, inverse, out, left, rhs_here, inv_here, turned, sem):
    copies = [
        own_columns(where, rhs, 0, rhs_here.at[0], sem.at[0]),
        own_columns(where, rhs, 1, rhs_here.at[1], sem.at[1]),
        own_inverse(where, inverse, 0, inv_here, sem.at[2]),
    ]
    for copy in copies:
        copy.wait()
    width = out.shape[1]
    mine = pl.ds(pl.multiple_of(where[2] * width, width), width)
    turned[0] = rhs_here[0].T
    turned[1] = rhs_here[1].T
    to_copies(out, solved_flat(inv_here, turned[0, mine] - total_of(pieces.at[:, 0])))
    left[...] = turned[1, mine] - total_of(pieces.at[:, 1])


def anc_second_kernel(
    where, own, oth, pat_own, pat_oth, values, left, inverse, out, top, buffer, sems, inv_here, sem
):
    copy = own_inverse(where, inverse, 1, inv_here, sem.at[0])
    slab = Slab((own, oth, pat_own, pat_oth, TOP), buffer, sems, 0, 0)
    copy.wait()
    slab.wait()
    residual = left[...]
    for half in range(2):
        first = first_block(where, half)
        for block in range(8):
            residual = residual - nt(values[first + block], slab.block(half, block))
    back = solved_back(inv_here, solved_flat(inv_here, residual).astype(F32))
    top[...] = back
    for half in range(2):
        first = first_block(where, half)
        for block in range(8):
            out[first + block] = nn(back, slab.block(half, block)).astype(BF16)


def anc_third_kernel(where, pieces, lower, top, inverse, out, inv_here, sem):
    own_inverse(where, inverse, 0, inv_here, sem.at[0]).wait()
    residual = lower[where[0]].astype(F32) - total_of(pieces)
    value = solved_back(inv_here, residual)
    for peer in range(out.shape[0]):
        out[peer, 0] = value
        out[peer, 1] = top[...]


def back_sums(where, moving, values, out):
    for half in range(2):
        first = first_block(where, half)
        for block in range(8):
            total = None
            for slab, value in zip(moving, values):
                term = nn(value, slab.block(half, block))
                total = term if total is None else total + term
            out[first + block] = total.astype(BF16)


def of_layers(pieces, at):
    value = pieces[:, at]
    return value.reshape(-1, value.shape[-1])


def back_first_kernel(slabs, where, own, oth, pat_own, pat_oth, anc, out, natural, buffer, sems):
    refs = (own, oth, pat_own, pat_oth, CROSS)
    moving = [Slab(refs, buffer, sems, index, place) for place, index in enumerate(slabs)]
    values = [of_layers(anc, at) for at in range(2)]
    for at in range(2):
        natural[at] = flipped(values[at]).astype(BF16)
    for slab in moving:
        slab.wait()
    back_sums(where, moving, values, out)


def back_kernel(level, cross_slabs, leaf_slabs, where, cross, leaf, anc, pieces, value, inverse, *rest):
    *earlier, out, solution, natural, buffer, sems, inv_here, sem = rest
    copy = own_inverse(where, inverse, level, inv_here, sem.at[0])
    moving = [Slab(leaf, buffer, sems, index, place) for place, index in enumerate(leaf_slabs)]
    moving += [
        Slab(cross, buffer, sems, index, len(leaf_slabs) + place)
        for place, index in enumerate(cross_slabs)
    ]
    copy.wait()
    now = solved_back(inv_here, flipped(value[where[0]]) - total_of(pieces))
    solution[...] = now
    natural[...] = flipped(now).astype(BF16)
    values = [now, *(e[...] for e in earlier), *(of_layers(anc, at) for at in range(2))]
    for slab in moving:
        slab.wait()
    back_sums(where, moving, values, out)


def back_body(level, cross_slabs, leaf_slabs, where, *refs):
    patterns, rest = refs[4:6], refs[6:]
    cross, leaf = (*refs[:2], *patterns, CROSS), (*refs[2:4], *patterns, LEAF)
    back_kernel(level, cross_slabs, leaf_slabs, where, cross, leaf, *rest)


def last_kernel(where, pieces, value, inverse, second, third, anc, out, inv_here, sem):
    own_inverse(where, inverse, 0, inv_here, sem.at[0]).wait()
    now = solved_back(inv_here, flipped(value[where[0]]) - total_of(pieces))
    out[0] = flipped(now).astype(BF16)
    out[1] = second[...]
    out[2] = third[...]
    out[3] = anc[0]
    out[4] = anc[1]


def join_kernel(where, mine, theirs, leaf, anc, sem):
    copies = []
    for at in range(5):
        for side, half in enumerate((mine, theirs)):
            col = where[1] if side == 0 else 1 - where[1]
            columns = pl.ds(pl.multiple_of(col * 128, 128), 128)
            target = leaf.at[0, at, :, columns] if at < 3 else anc.at[at - 3, :, columns]
            copies.append(fetch(half.at[at], target, sem.at[at, side]))
    for copy in copies:
        copy.wait()


def shape(*dims, dtype=BF16):
    return jax.ShapeDtypeStruct(dims, dtype)


def slab_scratch(count):
    return [pltpu.VMEM((count, 2, 256, 2048), BF16), pltpu.SemaphoreType.DMA((count, 2))]


RHS_SCRATCH = pltpu.VMEM((256, 128), F32)
INV_SCRATCH = pltpu.VMEM((2, TILE, TILE), BF16)


def sem_scratch(count):
    return pltpu.SemaphoreType.DMA((count,))


def call(name, body, outs, operands, scratch, slabs=0, out_specs=None, limit=8):
    specs, arrays = [], []
    for x in operands:
        far = isinstance(x, tuple)
        x = pltpu.with_memory_space_constraint(x[1], pltpu.HBM) if far else x
        specs.append(HBM if far else SMEM if x.dtype == jnp.int32 else VMEM)
        arrays.append(x)
    single = not isinstance(outs, list)
    shapes = [outs] if single else outs
    made = pl.pallas_call(
        body,
        out_shape=shapes,
        in_specs=specs,
        out_specs=out_specs or [VMEM] * len(shapes),
        scratch_shapes=scratch,
        compiler_params=pltpu.CompilerParams(vmem_limit_bytes=limit * 1024 * 1024),
        cost_estimate=pl.CostEstimate(
            flops=max(1, slabs) * SLAB_FLOPS, bytes_accessed=2**21 * max(1, slabs), transcendentals=0
        ),
        name=name,
    )(*arrays)
    return made[0] if single else made


def spread(x, axis):
    return lax.all_to_all(x, axis, split_axis=0, concat_axis=0, tiled=True)


def local(
    leaf_rhs, anc_rhs, leaf_tiles, cross_tiles, top_tiles, leaf_pattern, cross_pattern, top_pattern,
    leaf_inverse, anc_inverse,
):
    layers = lax.axis_size("layer")
    rows = lax.axis_size("row")
    width = 128 // layers
    where = jnp.stack(
        [lax.axis_index(axis).astype(jnp.int32) for axis in ("row", "col", "layer")]
    )
    patterns = jnp.concatenate(
        [leaf_pattern.reshape(-1), cross_pattern.reshape(-1), top_pattern.reshape(-1)]
    )
    pat_other = lax.ppermute(patterns, "col", SWAP)
    tiles = (leaf_tiles[0], cross_tiles[0].reshape(6, 256, 2048), top_tiles)
    leaf_other, cross_other, top_other = (lax.ppermute(x, "col", SWAP) for x in tiles)
    leaf_own, cross_own, top_own = (("hbm", x) for x in tiles)
    rhs, rhs_anc = ("hbm", leaf_rhs[0]), ("hbm", anc_rhs)
    inv, inv_anc = ("hbm", leaf_inverse[0]), ("hbm", anc_inverse)
    small = [RHS_SCRATCH, INV_SCRATCH, sem_scratch(2)]

    wide = shape(rows, 256, 128)
    flat = shape(rows, 128, 256)
    thin = shape(rows, width, 256)

    def gathered(block):
        return spread(block, "row").reshape(rows * 256, 128)

    block = call("y0", first_kernel, wide, (where, rhs, inv), small)
    block, pat_other = lax.optimization_barrier((block, pat_other))
    patterns = (patterns, pat_other)
    y0 = gathered(block)
    leaf = (leaf_own, leaf_other, *patterns)
    block = call(
        "y1", functools.partial(forward_kernel, 1, (0,)), wide, (where, *leaf, rhs, inv, y0),
        [*slab_scratch(1), *small], 1, limit=12,
    )
    block, top_other = lax.optimization_barrier((block, top_other))
    y1 = gathered(block)
    block = call(
        "y2", functools.partial(forward_kernel, 2, (1, 2)), wide, (where, *leaf, rhs, inv, y0, y1),
        [*slab_scratch(2), *small], 2, limit=16,
    )
    block, cross_other = lax.optimization_barrier((block, cross_other))
    y2 = gathered(block)
    cross = (cross_own, ("hbm", cross_other), *patterns)
    lower = spread(
        call("zs", cross_kernel, shape(layers, 2, width, 256), (where, *cross, y0, y1, y2),
             slab_scratch(6), 6, limit=24),
        "layer",
    )
    z0, left = call(
        "z0", anc_first_kernel, [thin, shape(width, 256, dtype=F32)], (where, lower, rhs_anc, inv_anc),
        [pltpu.VMEM((2, 256, 128), F32), INV_SCRATCH, pltpu.VMEM((2, 128, 256), F32), sem_scratch(3)],
    )
    z0 = spread(z0, "row")
    top = (top_own, ("hbm", top_other), *patterns)
    pieces, high = call(
        "z1", anc_second_kernel, [thin, shape(width, 256)], (where, *top, z0, left, inv_anc),
        [*slab_scratch(1), INV_SCRATCH, sem_scratch(1)], 1,
    )
    pieces = spread(pieces, "row")
    anc = call(
        "a0", anc_third_kernel, shape(layers, 2, width, 256), (where, pieces, z0, high, inv_anc),
        [INV_SCRATCH, sem_scratch(1)],
    )
    anc = spread(anc, "layer")
    pieces, natural = call(
        "b2", functools.partial(back_first_kernel, (2, 5)), [flat, shape(2, 256, 128)], (where, *cross, anc),
        slab_scratch(2), 2, limit=12,
    )
    pieces = spread(pieces, "row")
    both = (cross_own, ("hbm", cross_other), leaf_own, leaf_other, *patterns)
    solved_outs = [flat, shape(128, 256), shape(256, 128)]
    y2, y1, y0 = (y.reshape(rows, 256, 128) for y in (y2, y1, y0))
    pieces, x2, n2 = call(
        "b1", functools.partial(back_body, 2, (1, 4), (2,)), solved_outs,
        (where, *both, anc, pieces, y2, inv), [*slab_scratch(3), INV_SCRATCH, sem_scratch(1)], 3, limit=20,
    )
    pieces = spread(pieces, "row")
    pieces, _, n1 = call(
        "b0", functools.partial(back_body, 1, (0, 3), (0, 1)), solved_outs,
        (where, *both, anc, pieces, y1, inv, x2), [*slab_scratch(4), INV_SCRATCH, sem_scratch(1)], 4, limit=20,
    )
    pieces = spread(pieces, "row")
    mine = call(
        "x0", last_kernel, shape(5, 256, 128), (where, pieces, y0, inv, n1, n2, natural),
        [INV_SCRATCH, sem_scratch(1)],
    )
    theirs = lax.ppermute(mine, "col", SWAP)
    return tuple(
        call("join", join_kernel, [shape(1, 3, 256, 256), shape(2, 256, 256)], (where, mine, theirs),
             [pltpu.SemaphoreType.DMA((5, 2))], out_specs=[HBM, HBM])
    )


def solution(mesh):
    in_specs = (
        P("layer", None, "row", None),
        P(None, "row", None),
        P("layer", None, "row", "col"),
        P("layer", None, None, "row", "col"),
        P(None, "row", "col"),
        P("layer", None, "row", "col"),
        P("layer", None, None, "row", "col"),
        P(None, "row", "col"),
        P("layer", None, None, None, None),
        P(),
    )
    out_specs = (P("layer", None, "row", None), P(None, "row", None))
    return jax.shard_map(local, mesh=mesh, in_specs=in_specs, out_specs=out_specs, check_vma=False)
```

```python
import functools

import jax
import jax.numpy as jnp
from jax import lax
from jax.experimental import pallas as pl
from jax.experimental.pallas import tpu as pltpu
from jax.sharding import PartitionSpec as P

F32 = jnp.float32
BF16 = jnp.bfloat16
TILE = 128
LINES = 16
SWAP = [(0, 1), (1, 0)]
SLAB_FLOPS = 2 * 256 * 4096 * 128

VMEM = pl.BlockSpec(memory_space=pltpu.VMEM)
SMEM = pl.BlockSpec(memory_space=pltpu.SMEM)
HBM = pl.BlockSpec(memory_space=pltpu.HBM)


def nt(a, b):
    return lax.dot_general(a, b, (((1,), (1,)), ((), ())), preferred_element_type=F32)


def nn(a, b):
    return jnp.dot(a, b, preferred_element_type=F32)


def packed(value):
    return jnp.concatenate(
        [value[LINES * k : LINES * (k + 1)] for k in range(value.shape[0] // LINES)], axis=1
    )


def unpacked(value, width):
    return jnp.concatenate(
        [value[:, width * k : width * (k + 1)] for k in range(value.shape[1] // width)], axis=0
    )


def first_block(half):
    col = lax.axis_index("col")
    return (col if half == 0 else 1 - col) * 8


def product(pair, slab, values):
    total = None
    for half in range(2):
        first = first_block(half)
        column = jnp.concatenate([unpacked(values[first + b], TILE) for b in range(8)], axis=0)
        term = nn(pair[half][slab], column)
        total = term if total is None else total + term
    return total


def solved(inverse, residual):
    cut = residual.astype(BF16)
    return jnp.concatenate(
        [nn(inverse[s], cut[TILE * s : TILE * (s + 1)]) for s in range(2)], axis=0
    ).astype(BF16)


def solved_flat(inverse, residual):
    cut = residual.astype(BF16)
    return jnp.concatenate(
        [nt(cut[:, TILE * s : TILE * (s + 1)], inverse[s]) for s in range(2)], axis=1
    ).astype(BF16)


def solved_back(inverse, residual):
    cut = residual.astype(BF16)
    return jnp.concatenate(
        [nn(cut[:, TILE * s : TILE * (s + 1)], inverse[s]) for s in range(2)], axis=1
    ).astype(BF16)


def to_copies(out, value):
    for peer in range(out.shape[0]):
        out[peer] = value


def total_of(pieces):
    total = pieces[0].astype(F32)
    for peer in range(1, pieces.shape[0]):
        total = total + pieces[peer].astype(F32)
    return total


def flipped(value):
    return value.astype(F32).T


def fetch(source, target, sem):
    copy = pltpu.make_async_copy(source, target, sem)
    copy.start()
    return copy


def mask_in_place(tiles, slab, pattern, at):
    for upper in range(2):
        for k in range(16):
            place = (slab, pl.ds(TILE * upper, TILE), pl.ds(TILE * k, TILE))
            tile = tiles[place]
            tiles[place] = lax.select(pattern[(*at, upper, k)] != 0, tile, jnp.zeros_like(tile))


def first_kernel(
    leaf_rhs, anc_rhs, leaf_tiles, cross_tiles, top_tiles, leaf_pattern, cross_pattern, top_pattern,
    leaf_inverse, anc_inverse,
    block, leaf, cross, top, rhs, rhs_anc, inv, inv_anc, rhs_here, anc_here, turned, sem, tile_sem,
):
    row, col, layer = (lax.axis_index(axis) for axis in ("row", "col", "layer"))
    columns = pl.ds(pl.multiple_of(col * 128, 128), 128)
    two = pl.ds(2 * row, 2)
    urgent = [
        fetch(leaf_rhs.at[0, 0, :, columns], rhs_here, sem.at[0]),
        fetch(leaf_inverse.at[0, :, two], inv, sem.at[1]),
    ]
    moving = [fetch(leaf_tiles.at[0, p], leaf.at[p], tile_sem.at[p]) for p in range(3)]
    moving += [
        fetch(cross_tiles.at[0, a, s], cross.at[3 * a + s], tile_sem.at[3 + 3 * a + s])
        for a in range(2)
        for s in range(3)
    ]
    moving += [fetch(top_tiles.at[0], top.at[0], tile_sem.at[9])]
    later = [
        fetch(leaf_rhs.at[0, pl.ds(1, 2), :, columns], rhs, sem.at[2]),
        fetch(anc_rhs.at[:, :, columns], anc_here, sem.at[3]),
        fetch(anc_inverse.at[:, two], inv_anc, sem.at[4]),
    ]
    for copy in urgent:
        copy.wait()
    to_copies(block, packed(solved(inv.at[0], rhs_here[...])))
    for p in range(3):
        moving[p].wait()
        mask_in_place(leaf, p, leaf_pattern, (0, p))
    for a in range(2):
        for s in range(3):
            moving[3 + 3 * a + s].wait()
            mask_in_place(cross, 3 * a + s, cross_pattern, (0, a, s))
    moving[9].wait()
    mask_in_place(top, 0, top_pattern, (0,))
    for copy in later:
        copy.wait()
    width = rhs_anc.shape[1]
    mine = pl.ds(pl.multiple_of(layer * width, width), width)
    for a in range(2):
        turned[a] = anc_here[a].T
        rhs_anc[a] = turned[a, mine]


def forward_kernel(level, slabs, own, oth, rhs, inverse, *rest):
    *values, out = rest
    residual = rhs[level - 1]
    for slab, value in zip(slabs, values):
        residual = residual - product((own, oth), slab, value)
    to_copies(out, packed(solved(inverse.at[level], residual)))


def cross_kernel(own, oth, *rest):
    *values, out = rest
    layers, width, _ = out.shape
    for a in range(2):
        total = None
        for s, value in enumerate(values):
            term = product((own, oth), a * len(values) + s, value)
            total = term if total is None else total + term
        out[:, :, 256 * a : 256 * (a + 1)] = total.T.astype(BF16).reshape(layers, width, -1)


def anc_first_kernel(pieces, rhs, inverse, out, left):
    total = total_of(pieces)
    to_copies(out, solved_flat(inverse.at[0], rhs[0] - total[:, :256]))
    left[...] = rhs[1] - total[:, 256:]


def anc_second_kernel(own, oth, values, left, inverse, out, top):
    residual = left[...]
    for half, tiles in enumerate((own, oth)):
        first = first_block(half)
        for block in range(8):
            residual = residual - nt(
                values[first + block], tiles[0, :, 256 * block : 256 * (block + 1)]
            )
    here = inverse.at[1]
    back = solved_back(here, solved_flat(here, residual).astype(F32))
    top[...] = back
    for half, tiles in enumerate((own, oth)):
        first = first_block(half)
        for block in range(8):
            out[first + block] = nn(back, tiles[0, :, 256 * block : 256 * (block + 1)]).astype(BF16)


def anc_third_kernel(pieces, lower, top, inverse, out):
    residual = lower[lax.axis_index("row")].astype(F32) - total_of(pieces)
    value = jnp.concatenate([solved_back(inverse.at[0], residual), top[...]], axis=1)
    to_copies(out, value)


def back_sums(terms, out):
    for half in range(2):
        first = first_block(half)
        for block in range(8):
            total = None
            for pair, slab, value in terms:
                term = nn(value, pair[half][slab, :, 256 * block : 256 * (block + 1)])
                total = term if total is None else total + term
            out[first + block] = packed(total.astype(BF16))


def of_layers(pieces, at):
    value = pieces[:, :, 256 * at : 256 * (at + 1)]
    return value.reshape(-1, value.shape[-1])


def back_first_kernel(slabs, own, oth, anc, out, natural):
    values = [of_layers(anc, at) for at in range(2)]
    back_sums([((own, oth), slab, value) for slab, value in zip(slabs, values)], out)
    for at in range(2):
        natural[at] = flipped(values[at]).astype(BF16)


def residual_of(value, pieces):
    own = unpacked(value[lax.axis_index("row")], TILE)
    return flipped(own) - unpacked(total_of(pieces), 256)


def back_kernel(level, cross_slabs, leaf_slabs, cown, coth, lown, loth, anc, pieces, value, inverse, *rest):
    *earlier, out, solution, natural = rest
    now = solved_back(inverse.at[level], residual_of(value, pieces))
    terms = [((cown, coth), slab, of_layers(anc, at)) for at, slab in enumerate(cross_slabs)]
    known = [now, *(e[...] for e in earlier)]
    terms += [((lown, loth), slab, x) for slab, x in zip(leaf_slabs, known)]
    back_sums(terms, out)
    solution[...] = now
    natural[...] = flipped(now).astype(BF16)


def last_kernel(pieces, value, inverse, second, third, anc, out):
    out[0] = flipped(solved_back(inverse.at[0], residual_of(value, pieces))).astype(BF16)
    out[1] = second[...]
    out[2] = third[...]
    out[3] = anc[0]
    out[4] = anc[1]


def join_kernel(mine, theirs, leaf, anc, sem):
    copies = []
    col = lax.axis_index("col")
    for at in range(5):
        for side, half in enumerate((mine, theirs)):
            columns = pl.ds(pl.multiple_of((col if side == 0 else 1 - col) * 128, 128), 128)
            target = leaf.at[0, at, :, columns] if at < 3 else anc.at[at - 3, :, columns]
            copies.append(fetch(half.at[at], target, sem.at[at, side]))
    for copy in copies:
        copy.wait()


def shape(*dims, dtype=BF16):
    return jax.ShapeDtypeStruct(dims, dtype)


def call(name, body, outs, operands, slabs=0, scratch=(), in_specs=None, out_specs=None, limit=6):
    single = not isinstance(outs, list)
    shapes = [outs] if single else outs
    made = pl.pallas_call(
        body,
        out_shape=shapes,
        in_specs=in_specs or [VMEM] * len(operands),
        out_specs=out_specs or [VMEM] * len(shapes),
        scratch_shapes=scratch,
        compiler_params=pltpu.CompilerParams(vmem_limit_bytes=limit * 1024 * 1024),
        cost_estimate=pl.CostEstimate(
            flops=max(1, slabs) * SLAB_FLOPS, bytes_accessed=2**21 * max(1, slabs), transcendentals=0
        ),
        name=name,
    )(*operands)
    return made[0] if single else made


def spread(x, axis):
    return lax.all_to_all(x, axis, split_axis=0, concat_axis=0, tiled=True)


def local(*args):
    layers = lax.axis_size("layer")
    rows = lax.axis_size("row")
    width = 128 // layers
    wide = shape(rows, LINES, 256 * 128 // LINES)
    thin = shape(rows, width, 256)
    far = pltpu.HBM
    args = tuple(
        x if x.dtype == jnp.int32 else pltpu.with_memory_space_constraint(x, far) for x in args
    )
    block, leaf, cross, top, rhs, rhs_anc, inv, inv_anc = call(
        "y0", first_kernel,
        [wide, shape(3, 256, 2048), shape(6, 256, 2048), shape(1, 256, 2048), shape(2, 256, 128, dtype=F32),
         shape(2, width, 256, dtype=F32), shape(3, 2, TILE, TILE), shape(2, 2, TILE, TILE)],
        args, 4,
        [pltpu.VMEM((256, 128), F32), pltpu.VMEM((2, 256, 128), F32), pltpu.VMEM((2, 128, 256), F32),
         pltpu.SemaphoreType.DMA((5,)), pltpu.SemaphoreType.DMA((10,))],
        in_specs=[SMEM if x.dtype == jnp.int32 else HBM for x in args], limit=16,
    )
    leaf, top, cross = ((x, lax.ppermute(x, "col", SWAP)) for x in (leaf, top, cross))
    y0 = spread(block, "row")
    block = call(
        "y1", functools.partial(forward_kernel, 1, (0,)), wide, (*leaf, rhs, inv, y0), 1
    )
    block, top = lax.optimization_barrier((block, top))
    y1 = spread(block, "row")
    block = call(
        "y2", functools.partial(forward_kernel, 2, (1, 2)), wide, (*leaf, rhs, inv, y0, y1), 2
    )
    block, cross = lax.optimization_barrier((block, cross))
    y2 = spread(block, "row")
    lower = spread(
        call("zs", cross_kernel, shape(layers, width, 512), (*cross, y0, y1, y2), 6), "layer"
    )
    z0, left = call(
        "z0", anc_first_kernel, [thin, shape(width, 256, dtype=F32)], (lower, rhs_anc, inv_anc)
    )
    z0 = spread(z0, "row")
    pieces, high = call(
        "z1", anc_second_kernel, [thin, shape(width, 256)], (*top, z0, left, inv_anc), 1
    )
    pieces = spread(pieces, "row")
    anc = call("a0", anc_third_kernel, shape(layers, width, 512), (pieces, z0, high, inv_anc))
    anc = spread(anc, "layer")
    pieces, natural = call(
        "b2", functools.partial(back_first_kernel, (2, 5)), [wide, shape(2, 256, 128)], (*cross, anc), 2
    )
    pieces = spread(pieces, "row")
    outs = [wide, shape(128, 256), shape(256, 128)]
    pieces, x2, n2 = call(
        "b1", functools.partial(back_kernel, 2, (1, 4), (2,)), outs, (*cross, *leaf, anc, pieces, y2, inv), 3
    )
    pieces = spread(pieces, "row")
    pieces, _, n1 = call(
        "b0", functools.partial(back_kernel, 1, (0, 3), (0, 1)), outs, (*cross, *leaf, anc, pieces, y1, inv, x2), 4
    )
    pieces = spread(pieces, "row")
    mine = call("x0", last_kernel, shape(5, 256, 128), (pieces, y0, inv, n1, n2, natural))
    theirs = lax.ppermute(mine, "col", SWAP)
    return tuple(
        call("join", join_kernel, [shape(1, 3, 256, 256), shape(2, 256, 256)], (mine, theirs),
             scratch=[pltpu.SemaphoreType.DMA((5, 2))], out_specs=[HBM, HBM])
    )


def solution(mesh):
    in_specs = (
        P("layer", None, "row", None),
        P(None, "row", None),
        P("layer", None, "row", "col"),
        P("layer", None, None, "row", "col"),
        P(None, "row", "col"),
        P("layer", None, "row", "col"),
        P("layer", None, None, "row", "col"),
        P(None, "row", "col"),
        P("layer", None, None, None, None),
        P(),
    )
    out_specs = (P("layer", None, "row", None), P(None, "row", None))
    return jax.shard_map(local, mesh=mesh, in_specs=in_specs, out_specs=out_specs, check_vma=False)
```

```python
import functools

import jax
import jax.numpy as jnp
from jax import lax
from jax.experimental import pallas as pl
from jax.experimental.pallas import tpu as pltpu
from jax.sharding import PartitionSpec as P

F32 = jnp.float32
BF16 = jnp.bfloat16
TILE = 128
LINES = 16
SWAP = [(0, 1), (1, 0)]
HOLD_START, HOLD_MIDDLE = 4500, 4500
SLAB_FLOPS = 2 * 256 * 4096 * 128

VMEM = pl.BlockSpec(memory_space=pltpu.VMEM)
SMEM = pl.BlockSpec(memory_space=pltpu.SMEM)
HBM = pl.BlockSpec(memory_space=pltpu.HBM)
ANY = pl.BlockSpec(memory_space=pl.ANY)


def nt(a, b):
    return lax.dot_general(a, b, (((1,), (1,)), ((), ())), preferred_element_type=F32)


def nn(a, b):
    return jnp.dot(a, b, preferred_element_type=F32)


def packed(value):
    return jnp.concatenate(
        [value[LINES * k : LINES * (k + 1)] for k in range(value.shape[0] // LINES)], axis=1
    )


def unpacked(value, width):
    return jnp.concatenate(
        [value[:, width * k : width * (k + 1)] for k in range(value.shape[1] // width)], axis=0
    )


def first_block(half):
    col = lax.axis_index("col")
    return (col if half == 0 else 1 - col) * 8


def gathered_column(values, half):
    first = first_block(half)
    return jnp.concatenate([unpacked(values[first + b], TILE) for b in range(8)], axis=0)


def product(pair, slab, values):
    return sum(nn(pair[half][slab], gathered_column(values, half)) for half in range(2))


def solved(inverse, residual):
    cut = residual.astype(BF16)
    return jnp.concatenate(
        [nn(inverse[s], cut[TILE * s : TILE * (s + 1)]) for s in range(2)], axis=0
    ).astype(BF16)


def solved_flat(inverse, residual):
    cut = residual.astype(BF16)
    return jnp.concatenate(
        [nt(cut[:, TILE * s : TILE * (s + 1)], inverse[s]) for s in range(2)], axis=1
    ).astype(BF16)


def solved_back(inverse, residual):
    cut = residual.astype(BF16)
    return jnp.concatenate(
        [nn(cut[:, TILE * s : TILE * (s + 1)], inverse[s]) for s in range(2)], axis=1
    ).astype(BF16)


def to_copies(out, value):
    for peer in range(out.shape[0]):
        out[peer] = value


def total_of(pieces):
    total = pieces[0].astype(F32)
    for peer in range(1, pieces.shape[0]):
        total = total + pieces[peer].astype(F32)
    return total


def flipped(value):
    return value.astype(F32).T


def linger(core, nanos):
    @pl.when(lax.axis_index("col") == core)
    def _():
        pl.delay(nanos)


def fetch(source, target, sem):
    copy = pltpu.make_async_copy(source, target, sem)
    copy.start()
    return copy


def mask_in_place(tiles, slab, kept):
    grow = lax.broadcasted_iota(jnp.int32, (16, 2048), 1) // TILE
    grow = (grow == lax.broadcasted_iota(jnp.int32, (16, 2048), 0)).astype(BF16)
    lines = nn((kept != 0).astype(F32).astype(BF16), grow)
    for upper in range(2):
        mask = jnp.broadcast_to(lines[upper : upper + 1], (LINES, 2048)).astype(BF16)
        for k in range(TILE // LINES):
            place = pl.ds(TILE * upper + LINES * k, LINES)
            tiles[slab, place, :] = tiles[slab, place, :] * mask


def first_kernel(
    leaf_rhs, anc_rhs, leaf_tiles, cross_tiles, top_tiles, leaf_kept, cross_kept, top_kept,
    leaf_inverse, anc_inverse,
    block, leaf, cross, top, rhs, rhs_anc, inv, inv_anc, rhs_here, anc_here, turned,
    leaf_pattern, cross_pattern, top_pattern, sem, tile_sem,
):
    row, col, layer = (lax.axis_index(axis) for axis in ("row", "col", "layer"))
    columns = pl.ds(pl.multiple_of(col * 128, 128), 128)
    two = pl.ds(2 * row, 2)
    urgent = [
        fetch(leaf_rhs.at[0, 0, :, columns], rhs_here, sem.at[0]),
        fetch(leaf_inverse.at[0, :, two], inv, sem.at[1]),
    ]
    moving = [fetch(leaf_tiles.at[0, p], leaf.at[p], tile_sem.at[p]) for p in range(3)]
    moving += [
        fetch(cross_tiles.at[0, a, s], cross.at[3 * a + s], tile_sem.at[3 + 3 * a + s])
        for a in range(2)
        for s in range(3)
    ]
    moving += [fetch(top_tiles.at[0], top.at[0], tile_sem.at[9])]
    patterns = [
        fetch(leaf_kept, leaf_pattern, sem.at[5]),
        fetch(cross_kept, cross_pattern, sem.at[6]),
        fetch(top_kept, top_pattern, sem.at[7]),
    ]
    later = [
        fetch(leaf_rhs.at[0, pl.ds(1, 2), :, columns], rhs, sem.at[2]),
        fetch(anc_rhs.at[:, :, columns], anc_here, sem.at[3]),
        fetch(anc_inverse.at[:, two], inv_anc, sem.at[4]),
    ]
    for copy in urgent:
        copy.wait()
    to_copies(block, packed(solved(inv.at[0], rhs_here[...])))
    for copy in patterns:
        copy.wait()
    for p in range(3):
        moving[p].wait()
        mask_in_place(leaf, p, leaf_pattern[0, p])
    for a in range(2):
        for s in range(3):
            moving[3 + 3 * a + s].wait()
            mask_in_place(cross, 3 * a + s, cross_pattern[0, a, s])
    moving[9].wait()
    mask_in_place(top, 0, top_pattern[0])
    for copy in later:
        copy.wait()
    width = rhs_anc.shape[1]
    mine = pl.ds(pl.multiple_of(layer * width, width), width)
    for a in range(2):
        turned[a] = anc_here[a].T
        rhs_anc[a] = turned[a, mine]


def hold_kernel(block, out):
    del block, out
    linger(0, HOLD_START)


def forward_kernel(level, slabs, own, oth, rhs, inverse, *rest):
    *values, out = rest
    residual = rhs[level - 1]
    for slab, value in zip(slabs, values):
        residual = residual - product((own, oth), slab, value)
    to_copies(out, packed(solved(inverse.at[level], residual)))


def cross_kernel(own, oth, *rest):
    *values, out = rest
    layers, width, _ = out.shape
    totals = [None, None]
    for s, value in enumerate(values):
        for half, tiles in enumerate((own, oth)):
            column = gathered_column(value, half)
            for a in range(2):
                term = nn(tiles[a * len(values) + s], column)
                totals[a] = term if totals[a] is None else totals[a] + term
    for a in range(2):
        out[:, :, 256 * a : 256 * (a + 1)] = totals[a].T.astype(BF16).reshape(layers, width, -1)


def anc_first_kernel(pieces, rhs, inverse, out, left):
    total = total_of(pieces)
    to_copies(out, solved_flat(inverse.at[0], rhs[0] - total[:, :256]))
    left[...] = rhs[1] - total[:, 256:]


def anc_second_kernel(own, oth, values, left, inverse, out, top):
    residual = left[...]
    for half, tiles in enumerate((own, oth)):
        first = first_block(half)
        for block in range(8):
            residual = residual - nt(
                values[first + block], tiles[0, :, 256 * block : 256 * (block + 1)]
            )
    here = inverse.at[1]
    back = solved_back(here, solved_flat(here, residual).astype(F32))
    top[...] = back
    for half, tiles in enumerate((own, oth)):
        first = first_block(half)
        for block in range(8):
            out[first + block] = nn(back, tiles[0, :, 256 * block : 256 * (block + 1)]).astype(BF16)


def anc_third_kernel(pieces, lower, top, inverse, out):
    residual = lower[lax.axis_index("row")].astype(F32) - total_of(pieces)
    value = jnp.concatenate([solved_back(inverse.at[0], residual), top[...]], axis=1)
    to_copies(out, value)
    linger(1, HOLD_MIDDLE)


def back_sums(terms, out):
    for half in range(2):
        first = first_block(half)
        for block in range(8):
            total = None
            for pair, slab, value in terms:
                term = nn(value, pair[half][slab, :, 256 * block : 256 * (block + 1)])
                total = term if total is None else total + term
            out[first + block] = packed(total.astype(BF16))


def of_layers(pieces, at):
    value = pieces[:, :, 256 * at : 256 * (at + 1)]
    return value.reshape(-1, value.shape[-1])


def back_first_kernel(slabs, own, oth, anc, out, natural):
    values = [of_layers(anc, at) for at in range(2)]
    back_sums([((own, oth), slab, value) for slab, value in zip(slabs, values)], out)
    for at in range(2):
        natural[at] = flipped(values[at]).astype(BF16)


def residual_of(value, pieces):
    own = unpacked(value[lax.axis_index("row")], TILE)
    return flipped(own) - unpacked(total_of(pieces), 256)


def back_kernel(level, cross_slabs, leaf_slabs, cown, coth, lown, loth, anc, pieces, value, inverse, *rest):
    *earlier, out, solution, natural = rest
    now = solved_back(inverse.at[level], residual_of(value, pieces))
    terms = [((cown, coth), slab, of_layers(anc, at)) for at, slab in enumerate(cross_slabs)]
    known = [now, *(e[...] for e in earlier)]
    terms += [((lown, loth), slab, x) for slab, x in zip(leaf_slabs, known)]
    back_sums(terms, out)
    solution[...] = now
    natural[...] = flipped(now).astype(BF16)


def last_kernel(pieces, value, inverse, second, third, anc, out):
    out[0] = flipped(solved_back(inverse.at[0], residual_of(value, pieces))).astype(BF16)
    out[1] = second[...]
    out[2] = third[...]
    out[3] = anc[0]
    out[4] = anc[1]


def join_kernel(mine, theirs, leaf, anc, sem):
    copies = []
    col = lax.axis_index("col")
    for at in range(5):
        for side, half in enumerate((mine, theirs)):
            columns = pl.ds(pl.multiple_of((col if side == 0 else 1 - col) * 128, 128), 128)
            target = leaf.at[0, at, :, columns] if at < 3 else anc.at[at - 3, :, columns]
            copies.append(fetch(half.at[at], target, sem.at[at, side]))
    for copy in copies:
        copy.wait()


def shape(*dims, dtype=BF16):
    return jax.ShapeDtypeStruct(dims, dtype)


def call(name, body, outs, operands, slabs=0, scratch=(), in_specs=None, out_specs=None, limit=6, alias={}):
    single = not isinstance(outs, list)
    shapes = [outs] if single else outs
    made = pl.pallas_call(
        body,
        out_shape=shapes,
        in_specs=in_specs or [VMEM] * len(operands),
        out_specs=out_specs or [VMEM] * len(shapes),
        scratch_shapes=scratch,
        input_output_aliases=alias,
        compiler_params=pltpu.CompilerParams(vmem_limit_bytes=limit * 1024 * 1024),
        cost_estimate=pl.CostEstimate(
            flops=max(1, slabs) * SLAB_FLOPS, bytes_accessed=2**21 * max(1, slabs), transcendentals=0
        ),
        name=name,
    )(*operands)
    return made[0] if single else made


def spread(x, axis):
    return lax.all_to_all(x, axis, split_axis=0, concat_axis=0, tiled=True)


def local(*args):
    layers = lax.axis_size("layer")
    rows = lax.axis_size("row")
    width = 128 // layers
    wide = shape(rows, LINES, 256 * 128 // LINES)
    thin = shape(rows, width, 256)
    far = pltpu.HBM
    args = tuple(pltpu.with_memory_space_constraint(x, far) for x in args)
    block, leaf, cross, top, rhs, rhs_anc, inv, inv_anc = call(
        "y0", first_kernel,
        [wide, shape(3, 256, 2048), shape(6, 256, 2048), shape(1, 256, 2048), shape(2, 256, 128, dtype=F32),
         shape(2, width, 256, dtype=F32), shape(3, 2, TILE, TILE), shape(2, 2, TILE, TILE)],
        args, 4,
        [pltpu.VMEM((256, 128), F32), pltpu.VMEM((2, 256, 128), F32), pltpu.VMEM((2, 128, 256), F32),
         *(pltpu.VMEM(x.shape, jnp.int32) for x in args[5:8]), pltpu.SemaphoreType.DMA((8,)),
         pltpu.SemaphoreType.DMA((10,))],
        in_specs=[HBM] * len(args), limit=16,
    )
    leaf, top, cross = ((x, lax.ppermute(x, "col", SWAP)) for x in (leaf, top, cross))
    block = call("hold", hold_kernel, wide, (block,), in_specs=[ANY], out_specs=[ANY], alias={0: 0})
    y0 = spread(block, "row")
    block = call(
        "y1", functools.partial(forward_kernel, 1, (0,)), wide, (*leaf, rhs, inv, y0), 1
    )
    block, top = lax.optimization_barrier((block, top))
    y1 = spread(block, "row")
    block = call(
        "y2", functools.partial(forward_kernel, 2, (1, 2)), wide, (*leaf, rhs, inv, y0, y1), 2
    )
    block, cross = lax.optimization_barrier((block, cross))
    y2 = spread(block, "row")
    lower = spread(
        call("zs", cross_kernel, shape(layers, width, 512), (*cross, y0, y1, y2), 6), "layer"
    )
    z0, left = call(
        "z0", anc_first_kernel, [thin, shape(width, 256, dtype=F32)], (lower, rhs_anc, inv_anc)
    )
    z0 = spread(z0, "row")
    pieces, high = call(
        "z1", anc_second_kernel, [thin, shape(width, 256)], (*top, z0, left, inv_anc), 1
    )
    pieces = spread(pieces, "row")
    anc = call("a0", anc_third_kernel, shape(layers, width, 512), (pieces, z0, high, inv_anc))
    anc = spread(anc, "layer")
    pieces, natural = call(
        "b2", functools.partial(back_first_kernel, (2, 5)), [wide, shape(2, 256, 128)], (*cross, anc), 2
    )
    pieces = spread(pieces, "row")
    outs = [wide, shape(128, 256), shape(256, 128)]
    pieces, x2, n2 = call(
        "b1", functools.partial(back_kernel, 2, (1, 4), (2,)), outs, (*cross, *leaf, anc, pieces, y2, inv), 3
    )
    pieces = spread(pieces, "row")
    pieces, _, n1 = call(
        "b0", functools.partial(back_kernel, 1, (0, 3), (0, 1)), outs, (*cross, *leaf, anc, pieces, y1, inv, x2), 4
    )
    pieces = spread(pieces, "row")
    mine = call("x0", last_kernel, shape(5, 256, 128), (pieces, y0, inv, n1, n2, natural))
    theirs = lax.ppermute(mine, "col", SWAP)
    return tuple(
        call("join", join_kernel, [shape(1, 3, 256, 256), shape(2, 256, 256)], (mine, theirs),
             scratch=[pltpu.SemaphoreType.DMA((5, 2))], out_specs=[HBM, HBM])
    )


def solution(mesh):
    in_specs = (
        P("layer", None, "row", None),
        P(None, "row", None),
        P("layer", None, "row", "col"),
        P("layer", None, None, "row", "col"),
        P(None, "row", "col"),
        P("layer", None, "row", "col"),
        P("layer", None, None, "row", "col"),
        P(None, "row", "col"),
        P("layer", None, None, None, None),
        P(),
    )
    out_specs = (P("layer", None, "row", None), P(None, "row", None))
    return jax.shard_map(local, mesh=mesh, in_specs=in_specs, out_specs=out_specs, check_vma=False)
```

```python
import functools

import jax
import jax.numpy as jnp
from jax import lax
from jax.experimental import pallas as pl
from jax.experimental.pallas import tpu as pltpu
from jax.sharding import PartitionSpec as P

F32 = jnp.float32
BF16 = jnp.bfloat16
TILE = 128
LINES = 16
SWAP = [(0, 1), (1, 0)]
HOLD_START, HOLD_MIDDLE = 9500, 4000
SLAB_FLOPS = 2 * 256 * 4096 * 128

VMEM = pl.BlockSpec(memory_space=pltpu.VMEM)
SMEM = pl.BlockSpec(memory_space=pltpu.SMEM)
HBM = pl.BlockSpec(memory_space=pltpu.HBM)
ANY = pl.BlockSpec(memory_space=pl.ANY)


def nt(a, b):
    return lax.dot_general(a, b, (((1,), (1,)), ((), ())), preferred_element_type=F32)


def nn(a, b):
    return jnp.dot(a, b, preferred_element_type=F32)


def packed(value):
    return jnp.concatenate(
        [value[LINES * k : LINES * (k + 1)] for k in range(value.shape[0] // LINES)], axis=1
    )


def unpacked(value, width):
    return jnp.concatenate(
        [value[:, width * k : width * (k + 1)] for k in range(value.shape[1] // width)], axis=0
    )


def first_block(half):
    col = lax.axis_index("col")
    return (col if half == 0 else 1 - col) * 8


def gathered_column(values, half):
    first = first_block(half)
    return jnp.concatenate([unpacked(values[first + b], TILE) for b in range(8)], axis=0)


def product(pair, slab, values):
    return sum(nn(pair[half][slab], gathered_column(values, half)) for half in range(2))


def solved(inverse, residual):
    cut = residual.astype(BF16)
    return jnp.concatenate(
        [nn(inverse[s], cut[TILE * s : TILE * (s + 1)]) for s in range(2)], axis=0
    ).astype(BF16)


def solved_flat(inverse, residual):
    cut = residual.astype(BF16)
    return jnp.concatenate(
        [nt(cut[:, TILE * s : TILE * (s + 1)], inverse[s]) for s in range(2)], axis=1
    ).astype(BF16)


def solved_back(inverse, residual):
    cut = residual.astype(BF16)
    return jnp.concatenate(
        [nn(cut[:, TILE * s : TILE * (s + 1)], inverse[s]) for s in range(2)], axis=1
    ).astype(BF16)


def to_copies(out, value):
    for peer in range(out.shape[0]):
        out[peer] = value


def total_of(pieces):
    total = pieces[0].astype(F32)
    for peer in range(1, pieces.shape[0]):
        total = total + pieces[peer].astype(F32)
    return total


def flipped(value):
    return value.astype(F32).T


def linger(core, nanos):
    @pl.when(lax.axis_index("col") == core)
    def _():
        pl.delay(nanos)


def fetch(source, target, sem):
    copy = pltpu.make_async_copy(source, target, sem)
    copy.start()
    return copy


def grow_masks(patterns, masks):
    grow = lax.broadcasted_iota(jnp.int32, (16, 2048), 1) // TILE
    grow = (grow == lax.broadcasted_iota(jnp.int32, (16, 2048), 0)).astype(BF16)
    for p in range(patterns.shape[0]):
        lines = nn((patterns[p] != 0).astype(F32).astype(BF16), grow)
        for upper in range(2):
            masks[p, upper] = jnp.broadcast_to(lines[upper : upper + 1], (LINES, 2048)).astype(BF16)


def mask_in_place(tiles, slab, masks, at):
    for upper in range(2):
        mask = masks[at, upper]
        for k in range(TILE // LINES):
            place = pl.ds(TILE * upper + LINES * k, LINES)
            tiles[slab, place, :] = tiles[slab, place, :] * mask


def first_kernel(
    leaf_rhs, anc_rhs, leaf_tiles, cross_tiles, top_tiles, leaf_kept, cross_kept, top_kept,
    leaf_inverse, anc_inverse,
    block, leaf, cross, top, rhs, rhs_anc, inv, inv_anc, rhs_here, anc_here, turned,
    patterns, masks, sem, tile_sem,
):
    row, col, layer = (lax.axis_index(axis) for axis in ("row", "col", "layer"))
    columns = pl.ds(pl.multiple_of(col * 128, 128), 128)
    two = pl.ds(2 * row, 2)
    kept = [
        fetch(leaf_kept.at[0], patterns.at[pl.ds(0, 3)], sem.at[5]),
        fetch(cross_kept.at[0, 0], patterns.at[pl.ds(3, 3)], sem.at[6]),
        fetch(cross_kept.at[0, 1], patterns.at[pl.ds(6, 3)], sem.at[7]),
        fetch(top_kept, patterns.at[pl.ds(9, 1)], sem.at[8]),
    ]
    urgent = [
        fetch(leaf_rhs.at[0, 0, :, columns], rhs_here, sem.at[0]),
        fetch(leaf_inverse.at[0, :, two], inv, sem.at[1]),
    ]
    moving = [fetch(leaf_tiles.at[0, p], leaf.at[p], tile_sem.at[p]) for p in range(3)]
    moving += [
        fetch(cross_tiles.at[0, a, s], cross.at[3 * a + s], tile_sem.at[3 + 3 * a + s])
        for a in range(2)
        for s in range(3)
    ]
    moving += [fetch(top_tiles.at[0], top.at[0], tile_sem.at[9])]
    later = [
        fetch(leaf_rhs.at[0, pl.ds(1, 2), :, columns], rhs, sem.at[2]),
        fetch(anc_rhs.at[:, :, columns], anc_here, sem.at[3]),
        fetch(anc_inverse.at[:, two], inv_anc, sem.at[4]),
    ]
    for copy in (*kept, *urgent):
        copy.wait()
    grow_masks(patterns, masks)
    to_copies(block, packed(solved(inv.at[0], rhs_here[...])))
    places = [(leaf, p) for p in range(3)] + [(cross, p) for p in range(6)] + [(top, 0)]
    for at, (copy, (tiles, slab)) in enumerate(zip(moving, places)):
        copy.wait()
        mask_in_place(tiles, slab, masks, at)
    for copy in later:
        copy.wait()
    width = rhs_anc.shape[1]
    mine = pl.ds(pl.multiple_of(layer * width, width), width)
    for a in range(2):
        turned[a] = anc_here[a].T
        rhs_anc[a] = turned[a, mine]


def hold_kernel(block, out):
    del block, out
    linger(1, HOLD_START)


def forward_kernel(level, slabs, own, oth, rhs, inverse, *rest):
    *values, out = rest
    residual = rhs[level - 1]
    for slab, value in zip(slabs, values):
        residual = residual - product((own, oth), slab, value)
    to_copies(out, packed(solved(inverse.at[level], residual)))


def cross_kernel(own, oth, *rest):
    *values, out = rest
    layers, width, _ = out.shape
    totals = [None, None]
    for s, value in enumerate(values):
        for half, tiles in enumerate((own, oth)):
            column = gathered_column(value, half)
            for a in range(2):
                term = nn(tiles[a * len(values) + s], column)
                totals[a] = term if totals[a] is None else totals[a] + term
    for a in range(2):
        out[:, :, 256 * a : 256 * (a + 1)] = totals[a].T.astype(BF16).reshape(layers, width, -1)


def anc_first_kernel(pieces, rhs, inverse, out, left):
    total = total_of(pieces)
    to_copies(out, solved_flat(inverse.at[0], rhs[0] - total[:, :256]))
    left[...] = rhs[1] - total[:, 256:]


def anc_second_kernel(own, oth, values, left, inverse, out, top):
    residual = left[...]
    for half, tiles in enumerate((own, oth)):
        first = first_block(half)
        for block in range(8):
            residual = residual - nt(
                values[first + block], tiles[0, :, 256 * block : 256 * (block + 1)]
            )
    here = inverse.at[1]
    back = solved_back(here, solved_flat(here, residual).astype(F32))
    top[...] = back
    for half, tiles in enumerate((own, oth)):
        first = first_block(half)
        for block in range(8):
            out[first + block] = nn(back, tiles[0, :, 256 * block : 256 * (block + 1)]).astype(BF16)


def anc_third_kernel(pieces, lower, top, inverse, out):
    residual = lower[lax.axis_index("row")].astype(F32) - total_of(pieces)
    value = jnp.concatenate([solved_back(inverse.at[0], residual), top[...]], axis=1)
    to_copies(out, value)
    linger(0, HOLD_MIDDLE)


def back_sums(terms, out):
    for half in range(2):
        first = first_block(half)
        for block in range(8):
            total = None
            for pair, slab, value in terms:
                term = nn(value, pair[half][slab, :, 256 * block : 256 * (block + 1)])
                total = term if total is None else total + term
            out[first + block] = packed(total.astype(BF16))


def of_layers(pieces, at):
    value = pieces[:, :, 256 * at : 256 * (at + 1)]
    return value.reshape(-1, value.shape[-1])


def back_first_kernel(slabs, own, oth, anc, out, natural):
    values = [of_layers(anc, at) for at in range(2)]
    back_sums([((own, oth), slab, value) for slab, value in zip(slabs, values)], out)
    for at in range(2):
        natural[at] = flipped(values[at]).astype(BF16)


def residual_of(value, pieces):
    own = unpacked(value[lax.axis_index("row")], TILE)
    return flipped(own) - unpacked(total_of(pieces), 256)


def back_kernel(level, cross_slabs, leaf_slabs, cown, coth, lown, loth, anc, pieces, value, inverse, *rest):
    *earlier, out, solution, natural = rest
    now = solved_back(inverse.at[level], residual_of(value, pieces))
    terms = [((cown, coth), slab, of_layers(anc, at)) for at, slab in enumerate(cross_slabs)]
    known = [now, *(e[...] for e in earlier)]
    terms += [((lown, loth), slab, x) for slab, x in zip(leaf_slabs, known)]
    back_sums(terms, out)
    solution[...] = now
    natural[...] = flipped(now).astype(BF16)


def last_kernel(pieces, value, inverse, second, third, anc, out):
    out[0] = flipped(solved_back(inverse.at[0], residual_of(value, pieces))).astype(BF16)
    out[1] = second[...]
    out[2] = third[...]
    out[3] = anc[0]
    out[4] = anc[1]


def join_kernel(mine, theirs, leaf, anc, sem):
    copies = []
    col = lax.axis_index("col")
    for at in range(5):
        for side, half in enumerate((mine, theirs)):
            columns = pl.ds(pl.multiple_of((col if side == 0 else 1 - col) * 128, 128), 128)
            target = leaf.at[0, at, :, columns] if at < 3 else anc.at[at - 3, :, columns]
            copies.append(fetch(half.at[at], target, sem.at[at, side]))
    for copy in copies:
        copy.wait()


def shape(*dims, dtype=BF16):
    return jax.ShapeDtypeStruct(dims, dtype)


def call(name, body, outs, operands, slabs=0, scratch=(), in_specs=None, out_specs=None, limit=6, alias={}):
    single = not isinstance(outs, list)
    shapes = [outs] if single else outs
    made = pl.pallas_call(
        body,
        out_shape=shapes,
        in_specs=in_specs or [VMEM] * len(operands),
        out_specs=out_specs or [VMEM] * len(shapes),
        scratch_shapes=scratch,
        input_output_aliases=alias,
        compiler_params=pltpu.CompilerParams(vmem_limit_bytes=limit * 1024 * 1024),
        cost_estimate=pl.CostEstimate(
            flops=max(1, slabs) * SLAB_FLOPS, bytes_accessed=2**21 * max(1, slabs), transcendentals=0
        ),
        name=name,
    )(*operands)
    return made[0] if single else made


def spread(x, axis):
    return lax.all_to_all(x, axis, split_axis=0, concat_axis=0, tiled=True)


def local(*args):
    layers = lax.axis_size("layer")
    rows = lax.axis_size("row")
    width = 128 // layers
    wide = shape(rows, LINES, 256 * 128 // LINES)
    thin = shape(rows, width, 256)
    far = pltpu.HBM
    args = tuple(pltpu.with_memory_space_constraint(x, far) for x in args)
    block, leaf, cross, top, rhs, rhs_anc, inv, inv_anc = call(
        "y0", first_kernel,
        [wide, shape(3, 256, 2048), shape(6, 256, 2048), shape(1, 256, 2048), shape(2, 256, 128, dtype=F32),
         shape(2, width, 256, dtype=F32), shape(3, 2, TILE, TILE), shape(2, 2, TILE, TILE)],
        args, 4,
        [pltpu.VMEM((256, 128), F32), pltpu.VMEM((2, 256, 128), F32), pltpu.VMEM((2, 128, 256), F32),
         pltpu.VMEM((10, 2, 16), jnp.int32), pltpu.VMEM((10, 2, LINES, 2048), BF16), pltpu.SemaphoreType.DMA((9,)),
         pltpu.SemaphoreType.DMA((10,))],
        in_specs=[HBM] * len(args), limit=16,
    )
    leaf, top, cross = ((x, lax.ppermute(x, "col", SWAP)) for x in (leaf, top, cross))
    block = call("hold", hold_kernel, wide, (block,), in_specs=[ANY], out_specs=[ANY], alias={0: 0})
    y0 = spread(block, "row")
    block = call(
        "y1", functools.partial(forward_kernel, 1, (0,)), wide, (*leaf, rhs, inv, y0), 1
    )
    block, top = lax.optimization_barrier((block, top))
    y1 = spread(block, "row")
    block = call(
        "y2", functools.partial(forward_kernel, 2, (1, 2)), wide, (*leaf, rhs, inv, y0, y1), 2
    )
    block, cross = lax.optimization_barrier((block, cross))
    y2 = spread(block, "row")
    lower = spread(
        call("zs", cross_kernel, shape(layers, width, 512), (*cross, y0, y1, y2), 6), "layer"
    )
    z0, left = call(
        "z0", anc_first_kernel, [thin, shape(width, 256, dtype=F32)], (lower, rhs_anc, inv_anc)
    )
    z0 = spread(z0, "row")
    pieces, high = call(
        "z1", anc_second_kernel, [thin, shape(width, 256)], (*top, z0, left, inv_anc), 1
    )
    pieces = spread(pieces, "row")
    anc = call("a0", anc_third_kernel, shape(layers, width, 512), (pieces, z0, high, inv_anc))
    anc = spread(anc, "layer")
    pieces, natural = call(
        "b2", functools.partial(back_first_kernel, (2, 5)), [wide, shape(2, 256, 128)], (*cross, anc), 2
    )
    pieces = spread(pieces, "row")
    outs = [wide, shape(128, 256), shape(256, 128)]
    pieces, x2, n2 = call(
        "b1", functools.partial(back_kernel, 2, (1, 4), (2,)), outs, (*cross, *leaf, anc, pieces, y2, inv), 3
    )
    pieces = spread(pieces, "row")
    pieces, _, n1 = call(
        "b0", functools.partial(back_kernel, 1, (0, 3), (0, 1)), outs, (*cross, *leaf, anc, pieces, y1, inv, x2), 4
    )
    pieces = spread(pieces, "row")
    mine = call("x0", last_kernel, shape(5, 256, 128), (pieces, y0, inv, n1, n2, natural))
    theirs = lax.ppermute(mine, "col", SWAP)
    return tuple(
        call("join", join_kernel, [shape(1, 3, 256, 256), shape(2, 256, 256)], (mine, theirs),
             scratch=[pltpu.SemaphoreType.DMA((5, 2))], out_specs=[HBM, HBM])
    )


def solution(mesh):
    in_specs = (
        P("layer", None, "row", None),
        P(None, "row", None),
        P("layer", None, "row", "col"),
        P("layer", None, None, "row", "col"),
        P(None, "row", "col"),
        P("layer", None, "row", "col"),
        P("layer", None, None, "row", "col"),
        P(None, "row", "col"),
        P("layer", None, None, None, None),
        P(),
    )
    out_specs = (P("layer", None, "row", None), P(None, "row", None))
    return jax.shard_map(local, mesh=mesh, in_specs=in_specs, out_specs=out_specs, check_vma=False)
```

```python
import functools

import jax
import jax.numpy as jnp
from jax import lax
from jax.experimental import pallas as pl
from jax.experimental.pallas import tpu as pltpu
from jax.sharding import PartitionSpec as P

F32 = jnp.float32
BF16 = jnp.bfloat16
TILE = 128
LINES = 16
CROSS, TOP = 3, 9
SWAP = [(0, 1), (1, 0)]
HOLD_START, HOLD_MIDDLE = 9500, 4000
SLAB_FLOPS = 2 * 256 * 4096 * 128

VMEM = pl.BlockSpec(memory_space=pltpu.VMEM)
SMEM = pl.BlockSpec(memory_space=pltpu.SMEM)
HBM = pl.BlockSpec(memory_space=pltpu.HBM)
ANY = pl.BlockSpec(memory_space=pl.ANY)


def nt(a, b):
    return lax.dot_general(a, b, (((1,), (1,)), ((), ())), preferred_element_type=F32)


def nn(a, b):
    return jnp.dot(a, b, preferred_element_type=F32)


def packed(value):
    return jnp.concatenate(
        [value[LINES * k : LINES * (k + 1)] for k in range(value.shape[0] // LINES)], axis=1
    )


def unpacked(value, width):
    return jnp.concatenate(
        [value[:, width * k : width * (k + 1)] for k in range(value.shape[1] // width)], axis=0
    )


def first_block(half):
    col = lax.axis_index("col")
    return (col if half == 0 else 1 - col) * 8


def gathered_column(values, half):
    first = first_block(half)
    return jnp.concatenate([unpacked(values[first + b], TILE) for b in range(8)], axis=0)


def product(pair, slab, values):
    return sum(nn(pair[half][slab], gathered_column(values, half)) for half in range(2))


def solved(inverse, residual):
    cut = residual.astype(BF16)
    return jnp.concatenate(
        [nn(inverse[s], cut[TILE * s : TILE * (s + 1)]) for s in range(2)], axis=0
    ).astype(BF16)


def solved_flat(inverse, residual):
    cut = residual.astype(BF16)
    return jnp.concatenate(
        [nt(cut[:, TILE * s : TILE * (s + 1)], inverse[s]) for s in range(2)], axis=1
    ).astype(BF16)


def solved_back(inverse, residual):
    cut = residual.astype(BF16)
    return jnp.concatenate(
        [nn(cut[:, TILE * s : TILE * (s + 1)], inverse[s]) for s in range(2)], axis=1
    ).astype(BF16)


def to_copies(out, value):
    for peer in range(out.shape[0]):
        out[peer] = value


def total_of(pieces):
    total = pieces[0].astype(F32)
    for peer in range(1, pieces.shape[0]):
        total = total + pieces[peer].astype(F32)
    return total


def flipped(value):
    return value.astype(F32).T


def linger(core, nanos):
    @pl.when(lax.axis_index("col") == core)
    def _():
        pl.delay(nanos)


def fetch(source, target, sem):
    copy = pltpu.make_async_copy(source, target, sem)
    copy.start()
    return copy


def grow_masks(patterns, masks):
    grow = lax.broadcasted_iota(jnp.int32, (16, 2048), 1) // TILE
    grow = (grow == lax.broadcasted_iota(jnp.int32, (16, 2048), 0)).astype(BF16)
    for p in range(patterns.shape[0]):
        lines = nn((patterns[p] != 0).astype(F32).astype(BF16), grow)
        for upper in range(2):
            masks[p, upper] = jnp.broadcast_to(lines[upper : upper + 1], (LINES, 2048)).astype(BF16)


def mask_in_place(tiles, slab, masks):
    for upper in range(2):
        mask = masks[slab, upper]
        for k in range(TILE // LINES):
            place = pl.ds(TILE * upper + LINES * k, LINES)
            tiles[slab, place, :] = tiles[slab, place, :] * mask


def first_kernel(
    leaf_rhs, anc_rhs, leaf_tiles, cross_tiles, top_tiles, leaf_kept, cross_kept, top_kept,
    leaf_inverse, anc_inverse,
    block, tiles, rhs, rhs_anc, inv, inv_anc, rhs_here, anc_here, turned,
    patterns, masks, sem, tile_sem,
):
    row, col, layer = (lax.axis_index(axis) for axis in ("row", "col", "layer"))
    columns = pl.ds(pl.multiple_of(col * 128, 128), 128)
    two = pl.ds(2 * row, 2)
    kept = [
        fetch(leaf_kept.at[0], patterns.at[pl.ds(0, 3)], sem.at[5]),
        fetch(cross_kept.at[0, 0], patterns.at[pl.ds(3, 3)], sem.at[6]),
        fetch(cross_kept.at[0, 1], patterns.at[pl.ds(6, 3)], sem.at[7]),
        fetch(top_kept, patterns.at[pl.ds(9, 1)], sem.at[8]),
    ]
    urgent = [
        fetch(leaf_rhs.at[0, 0, :, columns], rhs_here, sem.at[0]),
        fetch(leaf_inverse.at[0, :, two], inv, sem.at[1]),
    ]
    moving = [
        fetch(leaf_tiles.at[0], tiles.at[pl.ds(0, 3)], tile_sem.at[0]),
        fetch(cross_tiles.at[0, 0], tiles.at[pl.ds(CROSS, 3)], tile_sem.at[1]),
        fetch(cross_tiles.at[0, 1], tiles.at[pl.ds(CROSS + 3, 3)], tile_sem.at[2]),
        fetch(top_tiles, tiles.at[pl.ds(TOP, 1)], tile_sem.at[3]),
    ]
    later = [
        fetch(leaf_rhs.at[0, pl.ds(1, 2), :, columns], rhs, sem.at[2]),
        fetch(anc_rhs.at[:, :, columns], anc_here, sem.at[3]),
        fetch(anc_inverse.at[:, two], inv_anc, sem.at[4]),
    ]
    for copy in (*kept, *urgent):
        copy.wait()
    grow_masks(patterns, masks)
    to_copies(block, packed(solved(inv.at[0], rhs_here[...])))
    for slab in range(10):
        if slab % 3 == 0:
            moving[slab // 3].wait()
        mask_in_place(tiles, slab, masks)
    for copy in later:
        copy.wait()
    width = rhs_anc.shape[1]
    mine = pl.ds(pl.multiple_of(layer * width, width), width)
    for a in range(2):
        turned[a] = anc_here[a].T
        rhs_anc[a] = turned[a, mine]


def hold_kernel(block, out):
    del block, out
    linger(1, HOLD_START)


def forward_kernel(level, slabs, own, oth, rhs, inverse, *rest):
    *values, out = rest
    residual = rhs[level - 1]
    for slab, value in zip(slabs, values):
        residual = residual - product((own, oth), slab, value)
    to_copies(out, packed(solved(inverse.at[level], residual)))


def cross_kernel(own, oth, *rest):
    *values, out = rest
    layers, width, _ = out.shape
    totals = [None, None]
    for s, value in enumerate(values):
        for half, tiles in enumerate((own, oth)):
            column = gathered_column(value, half)
            for a in range(2):
                term = nn(tiles[CROSS + a * len(values) + s], column)
                totals[a] = term if totals[a] is None else totals[a] + term
    for a in range(2):
        out[:, :, 256 * a : 256 * (a + 1)] = totals[a].T.astype(BF16).reshape(layers, width, -1)


def anc_first_kernel(pieces, rhs, inverse, out, left):
    total = total_of(pieces)
    to_copies(out, solved_flat(inverse.at[0], rhs[0] - total[:, :256]))
    left[...] = rhs[1] - total[:, 256:]


def anc_second_kernel(own, oth, values, left, inverse, out, top):
    residual = left[...]
    for half, tiles in enumerate((own, oth)):
        first = first_block(half)
        for block in range(8):
            residual = residual - nt(
                values[first + block], tiles[TOP, :, 256 * block : 256 * (block + 1)]
            )
    here = inverse.at[1]
    back = solved_back(here, solved_flat(here, residual).astype(F32))
    top[...] = back
    for half, tiles in enumerate((own, oth)):
        first = first_block(half)
        for block in range(8):
            out[first + block] = nn(back, tiles[TOP, :, 256 * block : 256 * (block + 1)]).astype(BF16)


def anc_third_kernel(pieces, lower, top, inverse, out):
    residual = lower[lax.axis_index("row")].astype(F32) - total_of(pieces)
    value = jnp.concatenate([solved_back(inverse.at[0], residual), top[...]], axis=1)
    to_copies(out, value)
    linger(0, HOLD_MIDDLE)


def back_sums(terms, out):
    for half in range(2):
        first = first_block(half)
        for block in range(8):
            total = None
            for pair, slab, value in terms:
                term = nn(value, pair[half][slab, :, 256 * block : 256 * (block + 1)])
                total = term if total is None else total + term
            out[first + block] = packed(total.astype(BF16))


def of_layers(pieces, at):
    value = pieces[:, :, 256 * at : 256 * (at + 1)]
    return value.reshape(-1, value.shape[-1])


def back_first_kernel(slabs, own, oth, anc, out, natural):
    values = [of_layers(anc, at) for at in range(2)]
    back_sums([((own, oth), slab, value) for slab, value in zip(slabs, values)], out)
    for at in range(2):
        natural[at] = flipped(values[at]).astype(BF16)


def residual_of(value, pieces):
    own = unpacked(value[lax.axis_index("row")], TILE)
    return flipped(own) - unpacked(total_of(pieces), 256)


def back_kernel(level, cross_slabs, leaf_slabs, own, oth, anc, pieces, value, inverse, *rest):
    *earlier, out, solution, natural = rest
    now = solved_back(inverse.at[level], residual_of(value, pieces))
    terms = [((own, oth), slab, of_layers(anc, at)) for at, slab in enumerate(cross_slabs)]
    known = [now, *(e[...] for e in earlier)]
    terms += [((own, oth), slab, x) for slab, x in zip(leaf_slabs, known)]
    back_sums(terms, out)
    solution[...] = now
    natural[...] = flipped(now).astype(BF16)


def last_kernel(pieces, value, inverse, second, third, anc, out):
    out[0] = flipped(solved_back(inverse.at[0], residual_of(value, pieces))).astype(BF16)
    out[1] = second[...]
    out[2] = third[...]
    out[3] = anc[0]
    out[4] = anc[1]


def join_kernel(mine, theirs, leaf, anc, sem):
    copies = []
    col = lax.axis_index("col")
    for at in range(5):
        for side, half in enumerate((mine, theirs)):
            columns = pl.ds(pl.multiple_of((col if side == 0 else 1 - col) * 128, 128), 128)
            target = leaf.at[0, at, :, columns] if at < 3 else anc.at[at - 3, :, columns]
            copies.append(fetch(half.at[at], target, sem.at[at, side]))
    for copy in copies:
        copy.wait()


def shape(*dims, dtype=BF16):
    return jax.ShapeDtypeStruct(dims, dtype)


def call(name, body, outs, operands, slabs=0, scratch=(), in_specs=None, out_specs=None, limit=6, alias={}):
    single = not isinstance(outs, list)
    shapes = [outs] if single else outs
    made = pl.pallas_call(
        body,
        out_shape=shapes,
        in_specs=in_specs or [VMEM] * len(operands),
        out_specs=out_specs or [VMEM] * len(shapes),
        scratch_shapes=scratch,
        input_output_aliases=alias,
        compiler_params=pltpu.CompilerParams(vmem_limit_bytes=limit * 1024 * 1024),
        cost_estimate=pl.CostEstimate(
            flops=max(1, slabs) * SLAB_FLOPS, bytes_accessed=2**21 * max(1, slabs), transcendentals=0
        ),
        name=name,
    )(*operands)
    return made[0] if single else made


def spread(x, axis):
    return lax.all_to_all(x, axis, split_axis=0, concat_axis=0, tiled=True)


def local(*args):
    layers = lax.axis_size("layer")
    rows = lax.axis_size("row")
    width = 128 // layers
    wide = shape(rows, LINES, 256 * 128 // LINES)
    thin = shape(rows, width, 256)
    far = pltpu.HBM
    args = tuple(pltpu.with_memory_space_constraint(x, far) for x in args)
    block, tiles, rhs, rhs_anc, inv, inv_anc = call(
        "y0", first_kernel,
        [wide, shape(10, 256, 2048), shape(2, 256, 128, dtype=F32),
         shape(2, width, 256, dtype=F32), shape(3, 2, TILE, TILE), shape(2, 2, TILE, TILE)],
        args, 4,
        [pltpu.VMEM((256, 128), F32), pltpu.VMEM((2, 256, 128), F32), pltpu.VMEM((2, 128, 256), F32),
         pltpu.VMEM((10, 2, 16), jnp.int32), pltpu.VMEM((10, 2, LINES, 2048), BF16), pltpu.SemaphoreType.DMA((9,)),
         pltpu.SemaphoreType.DMA((4,))],
        in_specs=[HBM] * len(args), limit=16,
    )
    tiles = (tiles, lax.ppermute(tiles, "col", SWAP))
    block = call("hold", hold_kernel, wide, (block,), in_specs=[ANY], out_specs=[ANY], alias={0: 0})
    y0 = spread(block, "row")
    block = call(
        "y1", functools.partial(forward_kernel, 1, (0,)), wide, (*tiles, rhs, inv, y0), 1
    )
    y1 = spread(block, "row")
    block = call(
        "y2", functools.partial(forward_kernel, 2, (1, 2)), wide, (*tiles, rhs, inv, y0, y1), 2
    )
    y2 = spread(block, "row")
    lower = spread(
        call("zs", cross_kernel, shape(layers, width, 512), (*tiles, y0, y1, y2), 6), "layer"
    )
    z0, left = call(
        "z0", anc_first_kernel, [thin, shape(width, 256, dtype=F32)], (lower, rhs_anc, inv_anc)
    )
    z0 = spread(z0, "row")
    pieces, high = call(
        "z1", anc_second_kernel, [thin, shape(width, 256)], (*tiles, z0, left, inv_anc), 1
    )
    pieces = spread(pieces, "row")
    anc = call("a0", anc_third_kernel, shape(layers, width, 512), (pieces, z0, high, inv_anc))
    anc = spread(anc, "layer")
    pieces, natural = call(
        "b2", functools.partial(back_first_kernel, (CROSS + 2, CROSS + 5)), [wide, shape(2, 256, 128)], (*tiles, anc), 2
    )
    pieces = spread(pieces, "row")
    outs = [wide, shape(128, 256), shape(256, 128)]
    pieces, x2, n2 = call(
        "b1", functools.partial(back_kernel, 2, (CROSS + 1, CROSS + 4), (2,)), outs, (*tiles, anc, pieces, y2, inv), 3
    )
    pieces = spread(pieces, "row")
    pieces, _, n1 = call(
        "b0", functools.partial(back_kernel, 1, (CROSS, CROSS + 3), (0, 1)), outs, (*tiles, anc, pieces, y1, inv, x2), 4
    )
    pieces = spread(pieces, "row")
    mine = call("x0", last_kernel, shape(5, 256, 128), (pieces, y0, inv, n1, n2, natural))
    theirs = lax.ppermute(mine, "col", SWAP)
    return tuple(
        call("join", join_kernel, [shape(1, 3, 256, 256), shape(2, 256, 256)], (mine, theirs),
             scratch=[pltpu.SemaphoreType.DMA((5, 2))], out_specs=[HBM, HBM])
    )


def solution(mesh):
    in_specs = (
        P("layer", None, "row", None),
        P(None, "row", None),
        P("layer", None, "row", "col"),
        P("layer", None, None, "row", "col"),
        P(None, "row", "col"),
        P("layer", None, "row", "col"),
        P("layer", None, None, "row", "col"),
        P(None, "row", "col"),
        P("layer", None, None, None, None),
        P(),
    )
    out_specs = (P("layer", None, "row", None), P(None, "row", None))
    return jax.shard_map(local, mesh=mesh, in_specs=in_specs, out_specs=out_specs, check_vma=False)
```

```python
import functools

import jax
import jax.numpy as jnp
from jax import lax
from jax.experimental import pallas as pl
from jax.experimental.pallas import tpu as pltpu
from jax.sharding import PartitionSpec as P

F32 = jnp.float32
BF16 = jnp.bfloat16
TILE = 128
LINES = 16
CROSS, TOP = 3, 9
SWAP = [(0, 1), (1, 0)]
HOLD_START, HOLD_MIDDLE = 9500, 3800
SLAB_FLOPS = 2 * 256 * 4096 * 128

VMEM = pl.BlockSpec(memory_space=pltpu.VMEM)
SMEM = pl.BlockSpec(memory_space=pltpu.SMEM)
HBM = pl.BlockSpec(memory_space=pltpu.HBM)
ANY = pl.BlockSpec(memory_space=pl.ANY)


def nt(a, b):
    return lax.dot_general(a, b, (((1,), (1,)), ((), ())), preferred_element_type=F32)


def nn(a, b):
    return jnp.dot(a, b, preferred_element_type=F32)


def packed(value):
    return jnp.concatenate(
        [value[LINES * k : LINES * (k + 1)] for k in range(value.shape[0] // LINES)], axis=1
    )


def unpacked(value, width):
    return jnp.concatenate(
        [value[:, width * k : width * (k + 1)] for k in range(value.shape[1] // width)], axis=0
    )


def first_block(half):
    col = lax.axis_index("col")
    return (col if half == 0 else 1 - col) * 8


def gathered_column(values, half):
    first = first_block(half)
    return jnp.concatenate([unpacked(values[first + b], TILE) for b in range(8)], axis=0)


def product(pair, slab, values):
    return sum(nn(pair[half][slab], gathered_column(values, half)) for half in range(2))


def solved(inverse, residual):
    cut = residual.astype(BF16)
    return jnp.concatenate(
        [nn(inverse[s], cut[TILE * s : TILE * (s + 1)]) for s in range(2)], axis=0
    ).astype(BF16)


def solved_flat(inverse, residual):
    cut = residual.astype(BF16)
    return jnp.concatenate(
        [nt(cut[:, TILE * s : TILE * (s + 1)], inverse[s]) for s in range(2)], axis=1
    ).astype(BF16)


def solved_back(inverse, residual):
    cut = residual.astype(BF16)
    return jnp.concatenate(
        [nn(cut[:, TILE * s : TILE * (s + 1)], inverse[s]) for s in range(2)], axis=1
    ).astype(BF16)


def to_copies(out, value):
    for peer in range(out.shape[0]):
        out[peer] = value


def total_of(pieces):
    total = pieces[0].astype(F32)
    for peer in range(1, pieces.shape[0]):
        total = total + pieces[peer].astype(F32)
    return total


def flipped(value):
    return value.astype(F32).T


def linger(core, nanos):
    @pl.when(lax.axis_index("col") == core)
    def _():
        pl.delay(nanos)


def fetch(source, target, sem):
    copy = pltpu.make_async_copy(source, target, sem)
    copy.start()
    return copy


def grow_masks(patterns, masks):
    grow = lax.broadcasted_iota(jnp.int32, (16, 2048), 1) // TILE
    grow = (grow == lax.broadcasted_iota(jnp.int32, (16, 2048), 0)).astype(BF16)
    for p in range(patterns.shape[0]):
        lines = nn((patterns[p] != 0).astype(F32).astype(BF16), grow)
        for upper in range(2):
            masks[p, upper] = jnp.broadcast_to(lines[upper : upper + 1], (LINES, 2048)).astype(BF16)


def mask_in_place(tiles, slab, masks):
    for upper in range(2):
        mask = masks[slab, upper]
        for k in range(TILE // LINES):
            place = pl.ds(TILE * upper + LINES * k, LINES)
            tiles[slab, place, :] = tiles[slab, place, :] * mask


def first_kernel(
    leaf_rhs, anc_rhs, leaf_tiles, cross_tiles, top_tiles, leaf_kept, cross_kept, top_kept,
    leaf_inverse, anc_inverse,
    block, tiles, rhs, rhs_anc, inv, inv_anc, rhs_here, anc_here, turned,
    patterns, masks, sem, tile_sem,
):
    row, col, layer = (lax.axis_index(axis) for axis in ("row", "col", "layer"))
    columns = pl.ds(pl.multiple_of(col * 128, 128), 128)
    two = pl.ds(2 * row, 2)
    kept = [
        fetch(leaf_kept.at[0], patterns.at[pl.ds(0, 3)], sem.at[5]),
        fetch(cross_kept.at[0, 0], patterns.at[pl.ds(3, 3)], sem.at[6]),
        fetch(cross_kept.at[0, 1], patterns.at[pl.ds(6, 3)], sem.at[7]),
        fetch(top_kept, patterns.at[pl.ds(9, 1)], sem.at[8]),
    ]
    urgent = [
        fetch(leaf_rhs.at[0, 0, :, columns], rhs_here, sem.at[0]),
        fetch(leaf_inverse.at[0, :, two], inv, sem.at[1]),
    ]
    moving = [
        fetch(leaf_tiles.at[0], tiles.at[pl.ds(0, 3)], tile_sem.at[0]),
        fetch(cross_tiles.at[0, 0], tiles.at[pl.ds(CROSS, 3)], tile_sem.at[1]),
        fetch(cross_tiles.at[0, 1], tiles.at[pl.ds(CROSS + 3, 3)], tile_sem.at[2]),
        fetch(top_tiles, tiles.at[pl.ds(TOP, 1)], tile_sem.at[3]),
    ]
    later = [
        fetch(leaf_rhs.at[0, pl.ds(1, 2), :, columns], rhs, sem.at[2]),
        fetch(anc_rhs.at[:, :, columns], anc_here, sem.at[3]),
        fetch(anc_inverse.at[:, two], inv_anc, sem.at[4]),
    ]
    for copy in kept:
        copy.wait()
    grow_masks(patterns, masks)
    for copy in urgent:
        copy.wait()
    to_copies(block, packed(solved(inv.at[0], rhs_here[...])))
    for slab in range(10):
        if slab % 3 == 0:
            moving[slab // 3].wait()
        mask_in_place(tiles, slab, masks)
    for copy in later:
        copy.wait()
    width = rhs_anc.shape[1]
    mine = pl.ds(pl.multiple_of(layer * width, width), width)
    for a in range(2):
        turned[a] = anc_here[a].T
        rhs_anc[a] = turned[a, mine]


def hold_kernel(block, out):
    del block, out
    linger(1, HOLD_START)


def forward_kernel(level, slabs, own, oth, rhs, inverse, *rest):
    *values, out = rest
    residual = rhs[level - 1]
    for slab, value in zip(slabs, values):
        residual = residual - product((own, oth), slab, value)
    to_copies(out, packed(solved(inverse.at[level], residual)))


def cross_kernel(own, oth, *rest):
    *values, out = rest
    layers, width, _ = out.shape
    totals = [None, None]
    for s, value in enumerate(values):
        for half, tiles in enumerate((own, oth)):
            column = gathered_column(value, half)
            for a in range(2):
                term = nn(tiles[CROSS + a * len(values) + s], column)
                totals[a] = term if totals[a] is None else totals[a] + term
    for a in range(2):
        out[:, :, 256 * a : 256 * (a + 1)] = totals[a].T.astype(BF16).reshape(layers, width, -1)


def anc_first_kernel(pieces, rhs, inverse, out, left):
    total = total_of(pieces)
    to_copies(out, solved_flat(inverse.at[0], rhs[0] - total[:, :256]))
    left[...] = rhs[1] - total[:, 256:]


def anc_second_kernel(own, oth, values, left, inverse, out, top):
    residual = left[...]
    for half, tiles in enumerate((own, oth)):
        first = first_block(half)
        for block in range(8):
            residual = residual - nt(
                values[first + block], tiles[TOP, :, 256 * block : 256 * (block + 1)]
            )
    here = inverse.at[1]
    back = solved_back(here, solved_flat(here, residual).astype(F32))
    top[...] = back
    for half, tiles in enumerate((own, oth)):
        first = first_block(half)
        for block in range(8):
            out[first + block] = nn(back, tiles[TOP, :, 256 * block : 256 * (block + 1)]).astype(BF16)


def anc_third_kernel(pieces, lower, top, inverse, y0, y1, y2, out, turned):
    residual = lower[lax.axis_index("row")].astype(F32) - total_of(pieces)
    value = jnp.concatenate([solved_back(inverse.at[0], residual), top[...]], axis=1)
    to_copies(out, value)
    for level, value in enumerate((y0, y1, y2)):
        turned[level] = flipped(unpacked(value[lax.axis_index("row")], TILE))
    linger(0, HOLD_MIDDLE)


def back_sums(terms, out):
    for half in range(2):
        first = first_block(half)
        for block in range(8):
            total = None
            for pair, slab, value in terms:
                term = nn(value, pair[half][slab, :, 256 * block : 256 * (block + 1)])
                total = term if total is None else total + term
            out[first + block] = packed(total.astype(BF16))


def of_layers(pieces, at):
    value = pieces[:, :, 256 * at : 256 * (at + 1)]
    return value.reshape(-1, value.shape[-1])


def back_first_kernel(slabs, own, oth, anc, out, natural):
    values = [of_layers(anc, at) for at in range(2)]
    back_sums([((own, oth), slab, value) for slab, value in zip(slabs, values)], out)
    for at in range(2):
        natural[at] = flipped(values[at]).astype(BF16)


def residual_of(value, pieces):
    return value - unpacked(total_of(pieces), 256)


def back_kernel(level, cross_slabs, leaf_slabs, own, oth, anc, pieces, value, inverse, *rest):
    *earlier, out, solution, natural = rest
    now = solved_back(inverse.at[level], residual_of(value[level], pieces))
    terms = [((own, oth), slab, of_layers(anc, at)) for at, slab in enumerate(cross_slabs)]
    known = [now, *(e[...] for e in earlier)]
    terms += [((own, oth), slab, x) for slab, x in zip(leaf_slabs, known)]
    back_sums(terms, out)
    solution[...] = now
    natural[...] = flipped(now).astype(BF16)


def last_kernel(pieces, value, inverse, second, third, anc, out):
    out[0] = flipped(solved_back(inverse.at[0], residual_of(value[0], pieces))).astype(BF16)
    out[1] = second[...]
    out[2] = third[...]
    out[3] = anc[0]
    out[4] = anc[1]


def join_kernel(mine, theirs, leaf, anc, sem):
    copies = []
    col = lax.axis_index("col")
    for at in range(5):
        for side, half in enumerate((mine, theirs)):
            columns = pl.ds(pl.multiple_of((col if side == 0 else 1 - col) * 128, 128), 128)
            target = leaf.at[0, at, :, columns] if at < 3 else anc.at[at - 3, :, columns]
            copies.append(fetch(half.at[at], target, sem.at[at, side]))
    for copy in copies:
        copy.wait()


def shape(*dims, dtype=BF16):
    return jax.ShapeDtypeStruct(dims, dtype)


def call(name, body, outs, operands, slabs=0, scratch=(), in_specs=None, out_specs=None, limit=6, alias={}):
    single = not isinstance(outs, list)
    shapes = [outs] if single else outs
    made = pl.pallas_call(
        body,
        out_shape=shapes,
        in_specs=in_specs or [VMEM] * len(operands),
        out_specs=out_specs or [VMEM] * len(shapes),
        scratch_shapes=scratch,
        input_output_aliases=alias,
        compiler_params=pltpu.CompilerParams(vmem_limit_bytes=limit * 1024 * 1024),
        cost_estimate=pl.CostEstimate(
            flops=max(1, slabs) * SLAB_FLOPS, bytes_accessed=2**21 * max(1, slabs), transcendentals=0
        ),
        name=name,
    )(*operands)
    return made[0] if single else made


def spread(x, axis):
    return lax.all_to_all(x, axis, split_axis=0, concat_axis=0, tiled=True)


def local(*args):
    layers = lax.axis_size("layer")
    rows = lax.axis_size("row")
    width = 128 // layers
    wide = shape(rows, LINES, 256 * 128 // LINES)
    thin = shape(rows, width, 256)
    far = pltpu.HBM
    args = tuple(pltpu.with_memory_space_constraint(x, far) for x in args)
    block, tiles, rhs, rhs_anc, inv, inv_anc = call(
        "y0", first_kernel,
        [wide, shape(10, 256, 2048), shape(2, 256, 128, dtype=F32),
         shape(2, width, 256, dtype=F32), shape(3, 2, TILE, TILE), shape(2, 2, TILE, TILE)],
        args, 4,
        [pltpu.VMEM((256, 128), F32), pltpu.VMEM((2, 256, 128), F32), pltpu.VMEM((2, 128, 256), F32),
         pltpu.VMEM((10, 2, 16), jnp.int32), pltpu.VMEM((10, 2, LINES, 2048), BF16), pltpu.SemaphoreType.DMA((9,)),
         pltpu.SemaphoreType.DMA((4,))],
        in_specs=[HBM] * len(args), limit=16,
    )
    tiles = (tiles, lax.ppermute(tiles, "col", SWAP))
    block = call("hold", hold_kernel, wide, (block,), in_specs=[ANY], out_specs=[ANY], alias={0: 0})
    y0 = spread(block, "row")
    block = call(
        "y1", functools.partial(forward_kernel, 1, (0,)), wide, (*tiles, rhs, inv, y0), 1
    )
    y1 = spread(block, "row")
    block = call(
        "y2", functools.partial(forward_kernel, 2, (1, 2)), wide, (*tiles, rhs, inv, y0, y1), 2
    )
    y2 = spread(block, "row")
    lower = spread(
        call("zs", cross_kernel, shape(layers, width, 512), (*tiles, y0, y1, y2), 6), "layer"
    )
    z0, left = call(
        "z0", anc_first_kernel, [thin, shape(width, 256, dtype=F32)], (lower, rhs_anc, inv_anc)
    )
    z0 = spread(z0, "row")
    pieces, high = call(
        "z1", anc_second_kernel, [thin, shape(width, 256)], (*tiles, z0, left, inv_anc), 1
    )
    pieces = spread(pieces, "row")
    anc, turned = call(
        "a0", anc_third_kernel, [shape(layers, width, 512), shape(3, 128, 256, dtype=F32)],
        (pieces, z0, high, inv_anc, y0, y1, y2),
    )
    anc = spread(anc, "layer")
    pieces, natural = call(
        "b2", functools.partial(back_first_kernel, (CROSS + 2, CROSS + 5)), [wide, shape(2, 256, 128)], (*tiles, anc), 2
    )
    pieces = spread(pieces, "row")
    outs = [wide, shape(128, 256), shape(256, 128)]
    pieces, x2, n2 = call(
        "b1", functools.partial(back_kernel, 2, (CROSS + 1, CROSS + 4), (2,)), outs, (*tiles, anc, pieces, turned, inv), 3
    )
    pieces = spread(pieces, "row")
    pieces, _, n1 = call(
        "b0", functools.partial(back_kernel, 1, (CROSS, CROSS + 3), (0, 1)), outs, (*tiles, anc, pieces, turned, inv, x2), 4
    )
    pieces = spread(pieces, "row")
    mine = call("x0", last_kernel, shape(5, 256, 128), (pieces, turned, inv, n1, n2, natural))
    theirs = lax.ppermute(mine, "col", SWAP)
    return tuple(
        call("join", join_kernel, [shape(1, 3, 256, 256), shape(2, 256, 256)], (mine, theirs),
             scratch=[pltpu.SemaphoreType.DMA((5, 2))], out_specs=[HBM, HBM])
    )


def solution(mesh):
    in_specs = (
        P("layer", None, "row", None),
        P(None, "row", None),
        P("layer", None, "row", "col"),
        P("layer", None, None, "row", "col"),
        P(None, "row", "col"),
        P("layer", None, "row", "col"),
        P("layer", None, None, "row", "col"),
        P(None, "row", "col"),
        P("layer", None, None, None, None),
        P(),
    )
    out_specs = (P("layer", None, "row", None), P(None, "row", None))
    return jax.shard_map(local, mesh=mesh, in_specs=in_specs, out_specs=out_specs, check_vma=False)
```
